32 devices in a mesh: grp: 2 (over y), depth: 4 (over x, core), shot: 4 (over z).
Axes of the slice: x: 2, y: 2, z: 4, core: 2. Of those that a mesh axis runs over, the one named last changes fastest.
Arguments:
- forward: bfloat16 [4, 8, 32, 32, 128], P(None, ('grp', 'shot'), 'depth'), parts along dimension 1, may hold values from -6 to 6
- adjoint_last: float32 [8, 32, 32, 128], P(('grp', 'shot'), 'depth'), parts along dimension 0, may hold values from -6 to 6
- adjoint_late: float32 [8, 32, 32, 128], P(('grp', 'shot'), 'depth'), parts along dimension 0, may hold values from -6 to 6
- residuals: float32 [8, 4, 256], P(('grp', 'shot')), parts along dimension 0, may hold values from -6 to 6
- source_cells: int32 [8, 3], P('grp'), parts along dimension 0, may hold values from 0 to 127, as said below
- receiver_cells: int32 [8, 256, 3], P('grp'), parts along dimension 0, may hold values from 0 to 127, as said below
- assignment: int32 [8], P('grp'), parts along dimension 0, may hold values from 0 to 3, each once
- model: float32 [6, 32, 16, 64], P(None, ('grp', 'depth'), 'shot'), parts along dimension 1, may hold values from -0.4 to 2, as said below
Outputs:
- adjoint_first: float32 [8, 32, 32, 128], P(('grp', 'shot'), 'depth'), parts along dimension 0
- gradients: float32 [6, 32, 16, 64], P(None, ('grp', 'depth'), 'shot'), parts along dimension 1
The draws below stay inside these ranges and needn't reach their ends.
There are 2 independent parts, one for each index of `grp`. The reference program is written for one: setup_inputs(seed, part) draws one part's arguments, and reference() takes and returns one part's arrays. A program takes and returns all parts, laid end to end along the dimension named above; each array names one. Nothing has to cross between parts.
Inputs may be any that keep to these rules, and one draw needn't show every extreme that they name: `source_cells`: each row holds the depth, second and third cell index of a source inside the grid of 32 x 32 x 128 cells. `receiver_cells`: each entry holds the depth, second and third cell index of a receiver inside the grid; receivers may share a cell. `assignment`: each survey row is used by exactly one shot. `model`: channel 0 (depth with depth) lies in 1 to 2; channels 1 and 2 (second with second, third with third) lie in 0.25 to 1; channels 3 to 5 (depth with second, depth with third, second with third) lie in -0.4 to 0.4.
All inputs are finite; a program needn't handle non-finite values.
Results may differ from the reference program's by a relative error of at most 0.0003.
Values sent between devices are 32-bit elements; how exact they have to be, the bound alone decides.
No kernel may reach another device: no remote copies, remote signals or barrier semaphores. Data moves between devices by JAX's collectives and lax.ppermute only.
A program may use at most 128 MiB of HBM per device.

```python
import math
import jax
import jax.numpy as jnp
from jax import lax

NX = 32
NY = 128
STEPS = 4
NREC = 256
MUTE = 3
NZ = 32
ZC = 16
XC = 16
YC = 64
SHOTS = 4


def draw_model(key, part):
    depth_key, side_key, second_key = jax.random.split(jax.random.fold_in(key, 17), 3)
    single = (1, ZC, XC, YC)
    double = (2, ZC, XC, YC)
    triple = (3, ZC, XC, YC)
    vertical = jnp.exp(jax.random.uniform(depth_key, single, jnp.float32, 0.0, math.log(2.0)))
    lateral = jnp.exp(jax.random.uniform(side_key, double, jnp.float32, math.log(0.25), 0.0))
    crossed = jax.random.uniform(second_key, triple, jnp.float32, -0.3, 0.3)
    return jnp.concatenate([vertical, lateral, crossed], axis=0)


def cell_columns(key, leading):
    depth_key, row_key, column_key = jax.random.split(key, 3)
    return jnp.stack([jax.random.randint(depth_key, leading, 0, NZ, dtype=jnp.int32), jax.random.randint(row_key, leading, 0, NX, dtype=jnp.int32), jax.random.randint(column_key, leading, 0, NY, dtype=jnp.int32)], axis=-1)


def draw_source_cells(key, part):
    return cell_columns(jax.random.fold_in(key, 23), (SHOTS,))


def draw_receiver_cells(key, part):
    return cell_columns(jax.random.fold_in(key, 29), (SHOTS, NREC))


def levels(stream_key, extent, pieces, least, top_value):
    loudness = 1.0
    for dim, shards_of in pieces:
        heights = jax.random.uniform(jax.random.fold_in(jax.random.fold_in(stream_key, 6), dim), (shards_of,), jnp.float32, least / len(pieces), top_value / len(pieces))
        loudness = loudness * jnp.repeat(jnp.exp(heights), extent[dim] // shards_of).reshape((-1,) + (1,) * (len(extent) - 1 - dim))
    return loudness


def centred(stream_key, shape, width, limit, cuts=(), kind=jnp.bfloat16):
    entries = jax.random.normal(stream_key, shape, jnp.float32) * width
    if len(cuts) > 0:
        entries = levels(stream_key, shape, cuts, -0.22, 0.18) * entries
    return jnp.clip(entries, min=-limit, max=limit).astype(kind)


def setup_inputs(seed: int = 0, part: int = 0) -> dict:
    streams_of = jax.random.split(jax.random.key(seed), 9)
    part_keys = jax.random.split(jax.random.fold_in(streams_of[8], part), 9)
    forward = centred(part_keys[0], (STEPS, SHOTS, NZ, NX, NY), 1.0, 6.0, ((1, 4), (2, 4)))
    adjoint_last = centred(part_keys[1], (SHOTS, NZ, NX, NY), 1.0, 6.0, ((0, 4), (1, 4)), jnp.float32)
    adjoint_late = centred(part_keys[2], (SHOTS, NZ, NX, NY), 1.0, 6.0, ((0, 4), (1, 4)), jnp.float32)
    residuals = centred(part_keys[3], (SHOTS, STEPS, NREC), 1.0, 6.0, ((0, 4),), jnp.float32)
    source_cells = draw_source_cells(jax.random.fold_in(jax.random.fold_in(streams_of[8], part), 71), part)
    receiver_cells = draw_receiver_cells(jax.random.fold_in(jax.random.fold_in(streams_of[8], part), 71), part)
    assignment = jax.random.permutation(part_keys[6], SHOTS).astype(jnp.int32)
    model = draw_model(jax.random.fold_in(jax.random.fold_in(streams_of[8], part), 71), part)
    return {"forward": forward, "adjoint_last": adjoint_last, "adjoint_late": adjoint_late, "residuals": residuals, "source_cells": source_cells, "receiver_cells": receiver_cells, "assignment": assignment, "model": model}


TIME_SQUARED = 0.2


def refine(coarse, dimension):
    coarse_count = coarse.shape[dimension]
    later_rows = lax.slice_in_dim(coarse, 1, coarse_count, axis=dimension)
    edge_row = lax.slice_in_dim(coarse, coarse_count - 1, coarse_count, axis=dimension)
    middle = (coarse + jnp.concatenate([later_rows, edge_row], axis=dimension)) * 0.5
    merged = jnp.stack([coarse, middle], axis=dimension + 1)
    new_shape = coarse.shape[:dimension] + (2 * coarse_count,) + coarse.shape[dimension + 1:]
    return merged.reshape(new_shape)


def coarsen(fine_cells, dimension):
    half_count = fine_cells.shape[dimension] // 2
    paired = fine_cells.reshape(fine_cells.shape[:dimension] + (half_count, 2) + fine_cells.shape[dimension + 1:])
    even_cells = lax.index_in_dim(paired, 0, dimension + 1, keepdims=False)
    odd_cells = lax.index_in_dim(paired, 1, dimension + 1, keepdims=False)
    first_odd = lax.slice_in_dim(odd_cells, 0, 1, axis=dimension)
    earlier = jnp.concatenate([jnp.zeros_like(first_odd), lax.slice_in_dim(odd_cells, 0, half_count - 1, axis=dimension)], axis=dimension)
    tail_part = jnp.concatenate([jnp.zeros_like(lax.slice_in_dim(odd_cells, 1, half_count, axis=dimension)), lax.slice_in_dim(odd_cells, half_count - 1, half_count, axis=dimension)], axis=dimension)
    return even_cells + 0.5 * odd_cells + 0.5 * earlier + 0.5 * tail_part


def window(padded, offsets):
    depth_step, row_step, column_step = offsets
    inner_depth = padded.shape[-3] - 2
    inner_rows = padded.shape[-2] - 2
    inner_columns = padded.shape[-1] - 2
    return padded[..., 1 + depth_step:1 + depth_step + inner_depth, 1 + row_step:1 + row_step + inner_rows, 1 + column_step:1 + column_step + inner_columns]


def derivatives(padded):
    centre = window(padded, (0, 0, 0))

    def second(offsets, opposite):
        return window(padded, offsets) - 2.0 * centre + window(padded, opposite)

    def cross(upper_one, upper_two, lower_one, lower_two):
        return (window(padded, upper_one) - window(padded, upper_two) - window(padded, lower_one) + window(padded, lower_two)) * 0.25

    return jnp.stack([
        second((1, 0, 0), (-1, 0, 0)),
        second((0, 1, 0), (0, -1, 0)),
        second((0, 0, 1), (0, 0, -1)),
        cross((1, 1, 0), (1, -1, 0), (-1, 1, 0), (-1, -1, 0)),
        cross((1, 0, 1), (1, 0, -1), (-1, 0, 1), (-1, 0, -1)),
        cross((0, 1, 1), (0, 1, -1), (0, -1, 1), (0, -1, -1)),
    ], axis=0)


def reference(forward, adjoint_last, adjoint_late, residuals, source_cells, receiver_cells, assignment, model):
    coefficients = refine(refine(refine(model, 1), 3), 2)
    depth_cells = jnp.arange(NZ, dtype=jnp.int32)
    row_cells = jnp.arange(NX, dtype=jnp.int32)
    column_cells = jnp.arange(NY, dtype=jnp.int32)

    def one_shot(summed, shot_index):
        geometry = assignment[shot_index]
        sources = source_cells[geometry]
        receivers = receiver_cells[geometry]
        flat_index = ((receivers[:, 0] * NX + receivers[:, 1]) * NY + receivers[:, 2]).astype(jnp.int32)
        current = adjoint_last[shot_index]
        previous = adjoint_late[shot_index]
        totals = jnp.zeros((6, NZ, NX, NY), jnp.float32)
        for step_index in range(STEPS):
            slopes = derivatives(jnp.pad(current, 1))
            totals = totals + forward[step_index, shot_index].astype(jnp.float32)[None] * slopes
            updated = 2.0 * current - previous + TIME_SQUARED * jnp.sum(coefficients * slopes, axis=0)
            updated = updated.reshape(-1).at[flat_index].add(residuals[shot_index, step_index]).reshape(current.shape)
            previous, current = current, updated
        muted = ((jnp.abs(depth_cells - sources[0]) <= MUTE)[:, None, None]
                 & (jnp.abs(row_cells - sources[1]) <= MUTE)[None, :, None]
                 & (jnp.abs(column_cells - sources[2]) <= MUTE)[None, None, :])
        kept = jnp.where(muted[None], jnp.zeros_like(totals), totals)
        summed = summed + coarsen(coarsen(coarsen(kept, 3), 2), 1)
        return summed, current

    start = jnp.zeros((6, ZC, XC, YC), jnp.float32)
    summed, finals = lax.scan(one_shot, start, jnp.arange(SHOTS, dtype=jnp.int32))
    return finals, summed / STEPS
```

```python
import functools

import jax
import jax.numpy as jnp
from jax import lax
from jax.experimental import pallas as pl
from jax.experimental.pallas import tpu as pltpu
from jax.sharding import PartitionSpec as P

MUTE = 3
TIME_SQUARED = 0.2
PAD = 8
VMEM = pl.BlockSpec(memory_space=pltpu.VMEM)
SMEM = pl.BlockSpec(memory_space=pltpu.SMEM)


def refine_matrix(coarse):
    row = lax.broadcasted_iota(jnp.int32, (coarse, 2 * coarse), 0)
    column = lax.broadcasted_iota(jnp.int32, (coarse, 2 * coarse), 1)
    here = column // 2
    after = jnp.minimum(here + 1, coarse - 1)
    odd = (column % 2) == 1
    at_here = jnp.where(row == here, 1.0, 0.0)
    at_after = jnp.where(row == after, 1.0, 0.0)
    return jnp.where(odd, 0.5 * (at_here + at_after), at_here).astype(jnp.float32)


def exact_dot(left, right, contract):
    return lax.dot_general(
        left,
        right,
        (contract, ((), ())),
        precision=lax.Precision.HIGHEST,
        preferred_element_type=jnp.float32,
    )


def even_depth():
    return lax.axis_index("depth") % 2 == 0


def pack_model(model_ref, own_ref, first_ref, second_ref, staged, *, reach):
    channels, depth_len, rows, _ = model_ref.shape
    for z in range(depth_len):
        for k in range(channels):
            at = (z * channels + k) * rows
            staged[at : at + rows, :] = model_ref[k, z]
    own_ref[...] = exact_dot(staged[...], refine_matrix(model_ref.shape[3]), ((1,), (0,)))
    part = reach * channels * rows
    total = depth_len * channels * rows
    even = even_depth()

    @pl.when(even)
    def _():
        first_ref[...] = own_ref[total - part : total, :]
        second_ref[...] = own_ref[0:part, :]

    @pl.when(jnp.logical_not(even))
    def _():
        first_ref[...] = own_ref[0:part, :]
        second_ref[...] = own_ref[total - part : total, :]


def pack_fields(current_ref, previous_ref, forward_ref, first_ref, second_ref, *, steps):
    depth_len = current_ref.shape[1]
    up, down = steps + 1, steps

    def fill_bottom(out):
        out[0:up] = current_ref[0, depth_len - up : depth_len]
        out[up : 2 * up - 1] = previous_ref[0, depth_len - up + 1 : depth_len]
        for i in range(steps):
            out[2 * up - 1 + i] = forward_ref[i, 0, depth_len - 1].astype(jnp.float32)

    def fill_top(out):
        out[0:down] = current_ref[0, 0:down]
        out[down : 2 * down - 1] = previous_ref[0, 0 : down - 1]

    even = even_depth()

    @pl.when(even)
    def _():
        fill_bottom(first_ref)
        fill_top(second_ref)

    @pl.when(jnp.logical_not(even))
    def _():
        fill_top(first_ref)
        fill_bottom(second_ref)


def join_model(own_ref, first_ref, second_ref, out_ref, *, layer, depth_count):
    part = first_ref.shape[0]
    own = own_ref.shape[0]
    out_ref[part : part + own, :] = own_ref[...]
    even = even_depth()
    last = lax.axis_index("depth") == depth_count - 1

    @pl.when(even)
    def _():
        out_ref[0:part, :] = second_ref[...]
        out_ref[part + own : 2 * part + own, :] = first_ref[...]

    @pl.when(jnp.logical_not(even))
    def _():
        out_ref[0:part, :] = first_ref[...]
        out_ref[part + own : 2 * part + own, :] = second_ref[...]

    @pl.when(last)
    def _():
        out_ref[part + own : part + own + layer, :] = own_ref[own - layer : own, :]


def injection(assign_ref, residual_ref, receiver_ref, out_ref, *, steps, depth_len, rows):
    receivers = receiver_ref.shape[2]
    columns = out_ref.shape[3]
    count = out_ref.shape[1]
    geometry = assign_ref[lax.axis_index("shot")]
    first = lax.axis_index("depth") * depth_len - steps
    depth = receiver_ref[0, pl.ds(geometry, 1), :] - first
    flat = depth * rows + receiver_ref[1, pl.ds(geometry, 1), :]
    flat = jnp.where((depth >= 0) & (depth < count), flat, -1)
    cells = lax.broadcasted_iota(jnp.int32, (count * rows, receivers), 0)
    one_hot = jnp.where(cells == flat, 1.0, 0.0).astype(jnp.bfloat16)
    lanes = lax.broadcasted_iota(jnp.int32, (columns, receivers), 0)
    here = lanes == receiver_ref[2, pl.ds(geometry, 1), :]
    for i in range(steps):
        left = residual_ref[0, i : i + 1, :]
        total = None
        for _ in range(3):
            rounded = left.astype(jnp.bfloat16).astype(jnp.float32)
            left = left - rounded
            values = jnp.where(here, rounded, 0.0).astype(jnp.bfloat16)
            product = lax.dot_general(
                one_hot, values, (((1,), (1,)), ((), ())), preferred_element_type=jnp.float32
            )
            total = product if total is None else total + product
        out_ref[i] = total.reshape(count, rows, columns)


def march(
    assign_ref,
    source_ref,
    current_ref,
    previous_ref,
    forward_ref,
    first_ref,
    second_ref,
    added_ref,
    *refs,
    steps,
    shots,
    depth_count,
    channels,
    reach,
):
    gathered = refs[:shots]
    final_ref = refs[shots]
    chunks = refs[shots + 1 : 2 * shots + 1]
    blocks, coarse, even_rows, odd_rows, fields, across, bend, totals, result = refs[2 * shots + 1 :]
    depth_len, rows, columns = current_ref.shape[1:]
    up, down = steps + 1, steps
    height = up + depth_len + down
    depth_index = lax.axis_index("depth")
    shot_index = lax.axis_index("shot")
    is_even = depth_index % 2 == 0
    is_top = depth_index == 0
    is_last = depth_index == depth_count - 1
    coarse_rows = rows // 2
    share = coarse_rows // shots
    layers = depth_len // 2 + 2 * reach

    rim = jnp.zeros((height, PAD, columns), jnp.float32)
    for b in range(2):
        fields[b, :, 0:PAD, :] = rim
        fields[b, :, PAD + rows : 2 * PAD + rows, :] = rim
    across[:, 0:PAD, :] = rim
    across[:, PAD + rows : 2 * PAD + rows, :] = rim
    inner = slice(PAD, PAD + rows)
    fields[0, up : up + depth_len, inner, :] = current_ref[0]
    fields[1, up : up + depth_len, inner, :] = previous_ref[0]

    def from_above(ref):
        fields[0, 0:up, inner, :] = ref[0:up]
        fields[1, 1:up, inner, :] = ref[up : 2 * up - 1]
        for i in range(steps):
            result[i] = ref[2 * up - 1 + i]

    def from_below(ref):
        fields[0, up + depth_len : height, inner, :] = ref[0:down]
        fields[1, up + depth_len : height - 1, inner, :] = ref[down : 2 * down - 1]

    @pl.when(is_even)
    def _():
        from_above(second_ref)
        from_below(first_ref)

    @pl.when(jnp.logical_not(is_even))
    def _():
        from_above(first_ref)
        from_below(second_ref)

    @pl.when(is_top)
    def _():
        for b in range(2):
            fields[b, 0:up, inner, :] = jnp.zeros((up, rows, columns), jnp.float32)

    @pl.when(is_last)
    def _():
        for b in range(2):
            fields[b, up + depth_len : height, inner, :] = jnp.zeros(
                (down, rows, columns), jnp.float32
            )

    for j in range(shots):
        blocks[j] = gathered[j][...]
    for z in range(layers):
        for k in range(channels):
            at = (z * channels + k) * share
            for b in range(shots):
                coarse[z, k, b * share : (b + 1) * share, :] = blocks[shot_index ^ b, at : at + share, :]
            coarse[z, k, coarse_rows : coarse_rows + 1, :] = coarse[
                z, k, coarse_rows - 1 : coarse_rows, :
            ]
            scale = TIME_SQUARED if k < 3 else 0.25 * TIME_SQUARED
            here = coarse[z, k, 0:coarse_rows, :]
            after = coarse[z, k, 1 : coarse_rows + 1, :]
            even_rows[z, k, pl.ds(0, coarse_rows, stride=2), :] = here * scale
            even_rows[z, k, pl.ds(1, coarse_rows, stride=2), :] = (here + after) * (0.5 * scale)
    for z in range(layers - 1):
        for k in range(channels):
            odd_rows[z, k] = (even_rows[z, k] + even_rows[z + 1, k]) * 0.5

    lane = lax.broadcasted_iota(jnp.int32, (rows, columns), 1)
    leftmost = lane == 0
    rightmost = lane == columns - 1

    for i in range(steps):
        now, old = i % 2, 1 - i % 2
        lowest, highest = i, height - 1 - i
        for e in range(lowest, highest + 1):
            value = fields[now, e, inner, :]
            right = jnp.where(rightmost, 0.0, pltpu.roll(value, columns - 1, 1))
            left = jnp.where(leftmost, 0.0, pltpu.roll(value, 1, 1))
            across[e, inner, :] = right - left
            bend[e] = right + left - 2.0 * value
        for e in range(lowest + 1, highest):
            counted = up - 1 <= e < up + depth_len
            stepped = i < steps - 1 or up <= e < up + depth_len
            if not (counted or stepped):
                continue
            value = fields[now, e, inner, :]
            twice = 2.0 * value
            before = slice(PAD - 1, PAD - 1 + rows)
            after = slice(PAD + 1, PAD + 1 + rows)
            slopes = [
                fields[now, e + 1, inner, :] - twice + fields[now, e - 1, inner, :],
                fields[now, e, after, :] - twice + fields[now, e, before, :],
                bend[e],
                (fields[now, e + 1, after, :] - fields[now, e + 1, before, :])
                - (fields[now, e - 1, after, :] - fields[now, e - 1, before, :]),
                across[e + 1, inner, :] - across[e - 1, inner, :],
                across[e, after, :] - across[e, before, :],
            ]
            if counted:
                if e < up:
                    weight = result[i]
                else:
                    weight = forward_ref[i, 0, e - up].astype(jnp.float32)
                for k in range(channels):
                    if i == 0:
                        totals[k, e - up + 1] = weight * slopes[k]
                    else:
                        totals[k, e - up + 1] += weight * slopes[k]
            if stepped:
                z = e - up + 2 * reach
                table = even_rows if z % 2 == 0 else odd_rows
                change = table[z // 2, 0] * slopes[0]
                for k in range(1, channels):
                    change = change + table[z // 2, k] * slopes[k]
                updated = twice - fields[old, e, inner, :] + change + added_ref[i, e - 1]
                if e < up:
                    updated = jnp.where(is_top, 0.0, updated)
                if e >= up + depth_len:
                    updated = jnp.where(is_last, 0.0, updated)
                if i < steps - 1:
                    fields[old, e, inner, :] = updated
                else:
                    final_ref[0, e - up] = updated

    geometry = assign_ref[shot_index]
    first = depth_index * depth_len
    row = lax.broadcasted_iota(jnp.int32, (rows, columns), 0)
    near = (jnp.abs(row - source_ref[geometry, 1]) <= MUTE) & (
        jnp.abs(lane - source_ref[geometry, 2]) <= MUTE
    )
    near = jnp.where(near, 1, 0)
    masks = []
    for e in range(depth_len + 1):
        close = jnp.abs(first + e - 1 - source_ref[geometry, 0]) <= MUTE
        masks.append(near * jnp.where(close, 1, 0) > 0)
    rim_scale = jnp.where(is_top, 0.0, 0.5)
    last_scale = jnp.where(is_last, 1.0, 0.5)
    half = depth_len // 2
    for k in range(channels):
        kept = [jnp.where(masks[e], 0.0, totals[k, e]) for e in range(depth_len + 1)]
        for z in range(half):
            above = kept[0] * rim_scale if z == 0 else kept[2 * z] * 0.5
            below = kept[2 * z + 2] * (last_scale if z == half - 1 else 0.5)
            layer = kept[2 * z + 1] + above + below
            slot = steps + 1 + (k * half + z) % 4
            result[slot] = layer
            even = result[slot, pl.ds(0, coarse_rows, stride=2), :]
            odd = 0.5 * result[slot, pl.ds(1, coarse_rows, stride=2), :]
            across[0, PAD : PAD + coarse_rows, :] = odd
            line = lax.broadcasted_iota(jnp.int32, (coarse_rows, columns), 0)
            tail = jnp.where(line == coarse_rows - 1, odd, 0.0)
            value = even + odd + across[0, PAD - 1 : PAD - 1 + coarse_rows, :] + tail
            if k >= 3:
                value = value * 0.25
            at = (k * half + z) * share
            for b in range(shots):
                blocks[b, at : at + share, :] = value[b * share : (b + 1) * share, :]
    for j in range(shots):
        chunks[j][...] = blocks[shot_index ^ j, 0 : channels * half * share, :]


def finish(*refs, steps):
    parts, out_ref = refs[:-1], refs[-1]
    channels, depth_len, rows, columns = out_ref.shape
    total = parts[0][...]
    for part in parts[1:]:
        total = total + part[...]
    coarse = exact_dot(total, refine_matrix(columns), ((1,), (1,))) / steps
    for k in range(channels):
        for z in range(depth_len):
            at = (k * depth_len + z) * rows
            out_ref[k, z] = coarse[at : at + rows, :]


def on_device(
    forward, adjoint_last, adjoint_late, residuals, source_cells, receiver_cells, assignment, model
):
    steps = forward.shape[0]
    shots_here, depth_len, rows, columns = adjoint_last.shape
    channels, coarse_len, share, coarse_columns = model.shape
    shots = lax.axis_size("shot")
    depth_count = lax.axis_size("depth")
    reach = (steps + 1) // 2
    assert shots_here == 1 and depth_count % 2 == 0 and shots & (shots - 1) == 0
    assert depth_len > steps and coarse_len >= reach and share * shots * 2 == rows
    f32 = jnp.float32
    shape = lambda *dims: jax.ShapeDtypeStruct(dims, f32)
    call = lambda body, count, outs, **more: pl.pallas_call(
        body,
        in_specs=[VMEM] * count,
        out_specs=jax.tree.map(lambda _: VMEM, outs),
        out_shape=outs,
        **more,
    )
    first_pairs = [(i, i ^ 1) for i in range(depth_count)]
    second_pairs = [(i, (i + 1 if i % 2 else i - 1) % depth_count) for i in range(depth_count)]

    part = reach * channels * share
    own_rows = coarse_len * channels * share
    own, model_first, model_second = call(
        functools.partial(pack_model, reach=reach),
        1,
        (shape(own_rows, columns), shape(part, columns), shape(part, columns)),
        scratch_shapes=[pltpu.VMEM((own_rows, coarse_columns), f32)],
        name="pack_model",
    )(model)
    model_second = lax.ppermute(model_second, "depth", second_pairs)
    model_first = lax.ppermute(model_first, "depth", first_pairs)
    halo = 3 * steps + 1
    field_first, field_second = call(
        functools.partial(pack_fields, steps=steps),
        3,
        (shape(halo, rows, columns), shape(halo, rows, columns)),
        name="pack_fields",
    )(adjoint_last, adjoint_late, forward)
    field_second = lax.ppermute(field_second, "depth", second_pairs)
    field_first = lax.ppermute(field_first, "depth", first_pairs)
    joined_rows = own_rows + 2 * part
    joined = call(
        functools.partial(join_model, layer=channels * share, depth_count=depth_count),
        3,
        shape(joined_rows, columns),
        name="join_model",
    )(own, model_first, model_second)
    swap = lambda array, j: lax.ppermute(array, "shot", [(i, i ^ j) for i in range(shots)])
    gathered = [joined] + [swap(joined, j) for j in range(1, shots)]
    height = depth_len + 2 * steps + 1
    added = pl.pallas_call(
        functools.partial(injection, steps=steps, depth_len=depth_len, rows=rows),
        in_specs=[SMEM, VMEM, VMEM],
        out_specs=VMEM,
        out_shape=shape(steps, height - 2, rows, columns),
        name="injection",
    )(assignment, residuals, receiver_cells.transpose(2, 0, 1))
    layers = coarse_len + 2 * reach
    chunk = shape(channels * coarse_len * share, columns)
    final, *chunks = pl.pallas_call(
        functools.partial(
            march,
            steps=steps,
            shots=shots,
            depth_count=depth_count,
            channels=channels,
            reach=reach,
        ),
        in_specs=[SMEM, SMEM] + [VMEM] * (6 + shots),
        out_specs=[VMEM] * (1 + shots),
        out_shape=[shape(1, depth_len, rows, columns)] + [chunk] * shots,
        scratch_shapes=[
            pltpu.VMEM((shots, joined_rows, columns), f32),
            pltpu.VMEM((layers, channels, rows // 2 + PAD, columns), f32),
            pltpu.VMEM((layers, channels, rows, columns), f32),
            pltpu.VMEM((layers - 1, channels, rows, columns), f32),
            pltpu.VMEM((2, height, rows + 2 * PAD, columns), f32),
            pltpu.VMEM((height, rows + 2 * PAD, columns), f32),
            pltpu.VMEM((height, rows, columns), f32),
            pltpu.VMEM((channels, depth_len + 1, rows, columns), f32),
            pltpu.VMEM((steps + 5, rows, columns), f32),
        ],
        name="march",
    )(
        assignment,
        source_cells,
        adjoint_last,
        adjoint_late,
        forward,
        field_first,
        field_second,
        added,
        *gathered,
    )
    parts = [chunks[0]] + [swap(chunks[j], j) for j in range(1, shots)]
    gradients = call(
        functools.partial(finish, steps=steps), shots, shape(*model.shape), name="finish"
    )(*parts)
    return final, gradients


def solution(mesh):
    placed = (
        P(None, ("grp", "shot"), "depth", None, None),
        P(("grp", "shot"), "depth", None, None),
        P(("grp", "shot"), "depth", None, None),
        P(("grp", "shot"), None, None),
        P("grp", None),
        P("grp", None, None),
        P("grp"),
        P(None, ("grp", "depth"), "shot", None),
    )
    return jax.shard_map(
        on_device,
        mesh=mesh,
        in_specs=placed,
        out_specs=(
            P(("grp", "shot"), "depth", None, None),
            P(None, ("grp", "depth"), "shot", None),
        ),
        check_vma=False,
    )
```

```python
import functools

import jax
import jax.numpy as jnp
from jax import lax
from jax.experimental import pallas as pl
from jax.experimental.pallas import tpu as pltpu
from jax.sharding import PartitionSpec as P

MUTE = 3
TIME_SQUARED = 0.2
PAD = 8
VMEM = pl.BlockSpec(memory_space=pltpu.VMEM)
SMEM = pl.BlockSpec(memory_space=pltpu.SMEM)
HBM = pl.BlockSpec(memory_space=pltpu.HBM)
LIMIT = pltpu.CompilerParams(vmem_limit_bytes=16 * 1024 * 1024)


def refine_matrix(coarse):
    row = lax.broadcasted_iota(jnp.int32, (coarse, 2 * coarse), 0)
    column = lax.broadcasted_iota(jnp.int32, (coarse, 2 * coarse), 1)
    here = column // 2
    after = jnp.minimum(here + 1, coarse - 1)
    odd = (column % 2) == 1
    at_here = jnp.where(row == here, 1.0, 0.0)
    at_after = jnp.where(row == after, 1.0, 0.0)
    return jnp.where(odd, 0.5 * (at_here + at_after), at_here).astype(jnp.float32)


def exact_dot(left, right, contract):
    return lax.dot_general(
        left,
        right,
        (contract, ((), ())),
        precision=lax.Precision.HIGHEST,
        preferred_element_type=jnp.float32,
    )


def even_depth():
    return lax.axis_index("depth") % 2 == 0


def pack(
    model_ref,
    current_ref,
    previous_ref,
    forward_ref,
    own_ref,
    model_first,
    model_second,
    field_first,
    field_second,
    block,
    staged,
    weights,
    sems,
    *,
    steps,
    reach,
):
    channels, coarse_len, rows, coarse_columns = block.shape
    depth_len = current_ref.shape[1]
    up, down = steps + 1, steps
    even = even_depth()
    model_copy = pltpu.make_async_copy(model_ref, block, sems.at[0])
    weight_copy = pltpu.make_async_copy(
        forward_ref.at[:, 0, depth_len - 1], weights, sems.at[1]
    )
    model_copy.start()
    weight_copy.start()

    def copies(bottom, top):
        return [
            pltpu.make_async_copy(
                current_ref.at[0, depth_len - up : depth_len], bottom.at[0:up], sems.at[2]
            ),
            pltpu.make_async_copy(
                previous_ref.at[0, depth_len - up + 1 : depth_len],
                bottom.at[up : 2 * up - 1],
                sems.at[3],
            ),
            pltpu.make_async_copy(current_ref.at[0, 0:down], top.at[0:down], sems.at[4]),
            pltpu.make_async_copy(
                previous_ref.at[0, 0 : down - 1], top.at[down : 2 * down - 1], sems.at[5]
            ),
        ]

    @pl.when(even)
    def _():
        for copy in copies(field_first, field_second):
            copy.start()

    @pl.when(jnp.logical_not(even))
    def _():
        for copy in copies(field_second, field_first):
            copy.start()

    model_copy.wait()
    for z in range(coarse_len):
        for k in range(channels):
            at = (z * channels + k) * rows
            staged[at : at + rows, :] = block[k, z]
    own_ref[...] = exact_dot(staged[...], refine_matrix(coarse_columns), ((1,), (0,)))
    part = reach * channels * rows
    total = coarse_len * channels * rows
    weight_copy.wait()

    @pl.when(even)
    def _():
        model_first[...] = own_ref[total - part : total, :]
        model_second[...] = own_ref[0:part, :]
        for i in range(steps):
            field_first[2 * up - 1 + i] = weights[i].astype(jnp.float32)
        for copy in copies(field_first, field_second):
            copy.wait()

    @pl.when(jnp.logical_not(even))
    def _():
        model_first[...] = own_ref[0:part, :]
        model_second[...] = own_ref[total - part : total, :]
        for i in range(steps):
            field_second[2 * up - 1 + i] = weights[i].astype(jnp.float32)
        for copy in copies(field_second, field_first):
            copy.wait()


def join_model(own_ref, first_ref, second_ref, out_ref, *, layer, depth_count):
    part = first_ref.shape[0]
    own = own_ref.shape[0]
    out_ref[part : part + own, :] = own_ref[...]
    even = even_depth()
    last = lax.axis_index("depth") == depth_count - 1

    @pl.when(even)
    def _():
        out_ref[0:part, :] = second_ref[...]
        out_ref[part + own : 2 * part + own, :] = first_ref[...]

    @pl.when(jnp.logical_not(even))
    def _():
        out_ref[0:part, :] = first_ref[...]
        out_ref[part + own : 2 * part + own, :] = second_ref[...]

    @pl.when(last)
    def _():
        out_ref[part + own : part + own + layer, :] = own_ref[own - layer : own, :]


def injection(assign_ref, residual_ref, receiver_ref, out_ref, *, steps, depth_len, rows):
    receivers = receiver_ref.shape[2]
    columns = out_ref.shape[3]
    count = out_ref.shape[1]
    geometry = assign_ref[lax.axis_index("shot")]
    first = lax.axis_index("depth") * depth_len - steps
    depth = receiver_ref[0, pl.ds(geometry, 1), :] - first
    flat = depth * rows + receiver_ref[1, pl.ds(geometry, 1), :]
    flat = jnp.where((depth >= 0) & (depth < count), flat, -1)
    cells = lax.broadcasted_iota(jnp.int32, (count * rows, receivers), 0)
    one_hot = jnp.where(cells == flat, 1.0, 0.0).astype(jnp.bfloat16)
    lanes = lax.broadcasted_iota(jnp.int32, (columns, receivers), 0)
    here = lanes == receiver_ref[2, pl.ds(geometry, 1), :]
    for i in range(steps):
        left = residual_ref[0, i : i + 1, :]
        total = None
        for _ in range(3):
            rounded = left.astype(jnp.bfloat16).astype(jnp.float32)
            left = left - rounded
            values = jnp.where(here, rounded, 0.0).astype(jnp.bfloat16)
            product = lax.dot_general(
                one_hot, values, (((1,), (1,)), ((), ())), preferred_element_type=jnp.float32
            )
            total = product if total is None else total + product
        out_ref[i] = total.reshape(count, rows, columns)


def slopes_at(field, across, bend, e, rows):
    inner = slice(PAD, PAD + rows)
    before = slice(PAD - 1, PAD - 1 + rows)
    after = slice(PAD + 1, PAD + 1 + rows)
    twice = 2.0 * field[e, inner, :]
    slopes = [
        field[e + 1, inner, :] - twice + field[e - 1, inner, :],
        field[e, after, :] - twice + field[e, before, :],
        bend[e],
        (field[e + 1, after, :] - field[e + 1, before, :])
        - (field[e - 1, after, :] - field[e - 1, before, :]),
        across[e + 1, inner, :] - across[e - 1, inner, :],
        across[e, after, :] - across[e, before, :],
    ]
    return twice, slopes


def columns_of(field, across, bend, lowest, highest, rows):
    columns = field.shape[2]
    inner = slice(PAD, PAD + rows)
    lane = lax.broadcasted_iota(jnp.int32, (rows, columns), 1)
    for e in range(lowest, highest + 1):
        value = field[e, inner, :]
        right = jnp.where(lane == columns - 1, 0.0, pltpu.roll(value, columns - 1, 1))
        left = jnp.where(lane == 0, 0.0, pltpu.roll(value, 1, 1))
        across[e, inner, :] = right - left
        bend[e] = right + left - 2.0 * value


def clear_rim(field, rows):
    height, _, columns = field.shape
    rim = jnp.zeros((height, PAD, columns), jnp.float32)
    field[:, 0:PAD, :] = rim
    field[:, PAD + rows : 2 * PAD + rows, :] = rim


def prepare(
    current_ref,
    previous_ref,
    forward_ref,
    first_ref,
    second_ref,
    added_ref,
    field,
    start_slopes,
    start_base,
    start_totals,
    weights,
    across,
    bend,
    older,
    *,
    steps,
    depth_count,
):
    depth_len, rows, _ = current_ref.shape[1:]
    up, down = steps + 1, steps
    height = up + depth_len + down
    depth_index = lax.axis_index("depth")
    is_even = depth_index % 2 == 0
    inner = slice(PAD, PAD + rows)
    clear_rim(field, rows)
    clear_rim(across, rows)
    field[up : up + depth_len, inner, :] = current_ref[0]
    older[up : up + depth_len] = previous_ref[0]
    for i in range(steps):
        weights[i, 1 : depth_len + 1] = forward_ref[i, 0].astype(jnp.float32)

    def from_above(ref):
        field[0:up, inner, :] = ref[0:up]
        older[1:up] = ref[up : 2 * up - 1]
        for i in range(steps):
            weights[i, 0] = ref[2 * up - 1 + i]

    def from_below(ref):
        field[up + depth_len : height, inner, :] = ref[0:down]
        older[up + depth_len : height - 1] = ref[down : 2 * down - 1]

    @pl.when(is_even)
    def _():
        from_above(second_ref)
        from_below(first_ref)

    @pl.when(jnp.logical_not(is_even))
    def _():
        from_above(first_ref)
        from_below(second_ref)

    @pl.when(depth_index == 0)
    def _():
        field[0:up, inner, :] = jnp.zeros((up,) + current_ref.shape[2:], jnp.float32)
        older[0:up] = jnp.zeros((up,) + current_ref.shape[2:], jnp.float32)

    @pl.when(depth_index == depth_count - 1)
    def _():
        field[up + depth_len : height, inner, :] = jnp.zeros(
            (down,) + current_ref.shape[2:], jnp.float32
        )
        older[up + depth_len : height] = jnp.zeros((down,) + current_ref.shape[2:], jnp.float32)

    columns_of(field, across, bend, 0, height - 1, rows)
    for e in range(1, height - 1):
        twice, slopes = slopes_at(field, across, bend, e, rows)
        for k, slope in enumerate(slopes):
            start_slopes[k, e - 1] = slope
            if up - 1 <= e < up + depth_len:
                start_totals[k, e - up + 1] = weights[0, e - up + 1] * slope
        start_base[e - 1] = twice - older[e] + added_ref[0, e - 1]


def march(
    assign_ref,
    source_ref,
    field,
    start_slopes,
    start_base,
    start_totals,
    weights,
    added_ref,
    *refs,
    steps,
    shots,
    depth_count,
    reach,
):
    gathered = refs[:shots]
    final_ref = refs[shots]
    chunks = refs[shots + 1 : 2 * shots + 1]
    blocks, coarse, even_rows, odd_rows, ones, twos, across, bend, totals, result = refs[
        2 * shots + 1 :
    ]
    depth_len, rows, columns = final_ref.shape[1:]
    channels = start_slopes.shape[0]
    up, down = steps + 1, steps
    height = up + depth_len + down
    depth_index = lax.axis_index("depth")
    shot_index = lax.axis_index("shot")
    is_top = depth_index == 0
    is_last = depth_index == depth_count - 1
    coarse_rows = rows // 2
    share = coarse_rows // shots
    layers = depth_len // 2 + 2 * reach
    inner = slice(PAD, PAD + rows)
    for scratch in (ones, twos, across):
        clear_rim(scratch, rows)

    for j in range(shots):
        blocks[j] = gathered[j][...]
    for z in range(layers):
        for k in range(channels):
            at = (z * channels + k) * share
            for b in range(shots):
                coarse[z, k, b * share : (b + 1) * share, :] = blocks[
                    shot_index ^ b, at : at + share, :
                ]
            coarse[z, k, coarse_rows : coarse_rows + 1, :] = coarse[
                z, k, coarse_rows - 1 : coarse_rows, :
            ]
            scale = TIME_SQUARED if k < 3 else 0.25 * TIME_SQUARED
            here = coarse[z, k, 0:coarse_rows, :]
            after = coarse[z, k, 1 : coarse_rows + 1, :]
            even_rows[z, k, pl.ds(0, coarse_rows, stride=2), :] = here * scale
            even_rows[z, k, pl.ds(1, coarse_rows, stride=2), :] = (here + after) * (0.5 * scale)
    for z in range(layers - 1):
        for k in range(channels):
            odd_rows[z, k] = (even_rows[z, k] + even_rows[z + 1, k]) * 0.5

    for i in range(steps):
        now = field if i == 0 else (ones if i % 2 else twos)
        old = field if i == 1 else (twos if i % 2 else ones)
        new = twos if i % 2 else ones
        if i > 0:
            columns_of(now, across, bend, i, height - 1 - i, rows)
        for e in range(i + 1, height - 1 - i):
            counted = up - 1 <= e < up + depth_len and i > 0
            stepped = i < steps - 1 or up <= e < up + depth_len
            if not (counted or stepped):
                continue
            if i == 0:
                slopes = [start_slopes[k, e - 1] for k in range(channels)]
                base = start_base[e - 1]
            else:
                twice, slopes = slopes_at(now, across, bend, e, rows)
            if counted:
                weight = weights[i, e - up + 1]
                for k in range(channels):
                    so_far = start_totals if i == 1 else totals
                    totals[k, e - up + 1] = so_far[k, e - up + 1] + weight * slopes[k]
            if stepped:
                if i > 0:
                    base = twice - old[e, inner, :] + added_ref[i, e - 1]
                z = e - up + 2 * reach
                table = even_rows if z % 2 == 0 else odd_rows
                change = table[z // 2, 0] * slopes[0]
                for k in range(1, channels):
                    change = change + table[z // 2, k] * slopes[k]
                updated = base + change
                if e < up:
                    updated = jnp.where(is_top, 0.0, updated)
                if e >= up + depth_len:
                    updated = jnp.where(is_last, 0.0, updated)
                if i < steps - 1:
                    new[e, inner, :] = updated
                else:
                    final_ref[0, e - up] = updated
    if steps == 1:
        totals[...] = start_totals[...]

    geometry = assign_ref[shot_index]
    first = depth_index * depth_len
    row = lax.broadcasted_iota(jnp.int32, (rows, columns), 0)
    lane = lax.broadcasted_iota(jnp.int32, (rows, columns), 1)
    near = (jnp.abs(row - source_ref[geometry, 1]) <= MUTE) & (
        jnp.abs(lane - source_ref[geometry, 2]) <= MUTE
    )
    near = jnp.where(near, 1, 0)
    masks = []
    for e in range(depth_len + 1):
        close = jnp.abs(first + e - 1 - source_ref[geometry, 0]) <= MUTE
        masks.append(near * jnp.where(close, 1, 0) > 0)
    rim_scale = jnp.where(is_top, 0.0, 0.5)
    last_scale = jnp.where(is_last, 1.0, 0.5)
    half = depth_len // 2
    line = lax.broadcasted_iota(jnp.int32, (coarse_rows, columns), 0)
    for k in range(channels):
        kept = [jnp.where(masks[e], 0.0, totals[k, e]) for e in range(depth_len + 1)]
        for z in range(half):
            above = kept[0] * rim_scale if z == 0 else kept[2 * z] * 0.5
            below = kept[2 * z + 2] * (last_scale if z == half - 1 else 0.5)
            slot = (k * half + z) % result.shape[0]
            result[slot] = kept[2 * z + 1] + above + below
            even = result[slot, pl.ds(0, coarse_rows, stride=2), :]
            odd = 0.5 * result[slot, pl.ds(1, coarse_rows, stride=2), :]
            ones[slot, PAD : PAD + coarse_rows, :] = odd
            tail = jnp.where(line == coarse_rows - 1, odd, 0.0)
            value = even + odd + ones[slot, PAD - 1 : PAD - 1 + coarse_rows, :] + tail
            if k >= 3:
                value = value * 0.25
            at = (k * half + z) * share
            for b in range(shots):
                blocks[b, at : at + share, :] = value[b * share : (b + 1) * share, :]
    for j in range(shots):
        chunks[j][...] = blocks[shot_index ^ j, 0 : channels * half * share, :]


def finish(*refs, steps):
    parts, out_ref = refs[:-1], refs[-1]
    channels, depth_len, rows, columns = out_ref.shape
    total = parts[0][...]
    for part in parts[1:]:
        total = total + part[...]
    coarse = exact_dot(total, refine_matrix(columns), ((1,), (1,))) / steps
    for k in range(channels):
        for z in range(depth_len):
            at = (k * depth_len + z) * rows
            out_ref[k, z] = coarse[at : at + rows, :]


def local_part(
    forward, adjoint_last, adjoint_late, residuals, source_cells, receiver_cells, assignment, model
):
    steps = forward.shape[0]
    shots_here, depth_len, rows, columns = adjoint_last.shape
    channels, coarse_len, share, coarse_columns = model.shape
    shots = lax.axis_size("shot")
    depth_count = lax.axis_size("depth")
    reach = (steps + 1) // 2
    assert shots_here == 1 and depth_count % 2 == 0 and shots & (shots - 1) == 0
    assert depth_len > steps and coarse_len >= reach and share * shots * 2 == rows
    f32 = jnp.float32
    shape = lambda *dims: jax.ShapeDtypeStruct(dims, f32)
    local = lambda *dims: pltpu.VMEM(dims, f32)
    near = lambda array: pltpu.with_memory_space_constraint(array, pltpu.VMEM)
    far = lambda array: pltpu.with_memory_space_constraint(array, pltpu.HBM)
    first_pairs = [(i, i ^ 1) for i in range(depth_count)]
    second_pairs = [(i, (i + 1 if i % 2 else i - 1) % depth_count) for i in range(depth_count)]

    def moved(array, axis, pairs):
        return near(lax.ppermute(array, axis, pairs))

    part = reach * channels * share
    own_rows = coarse_len * channels * share
    halo = 3 * steps + 1
    own, model_first, model_second, field_first, field_second = pl.pallas_call(
        functools.partial(pack, steps=steps, reach=reach),
        in_specs=[HBM] * 4,
        out_specs=[VMEM] * 5,
        out_shape=[
            local(own_rows, columns),
            local(part, columns),
            local(part, columns),
            local(halo, rows, columns),
            local(halo, rows, columns),
        ],
        scratch_shapes=[
            pltpu.VMEM((channels, coarse_len, share, coarse_columns), f32),
            pltpu.VMEM((own_rows, coarse_columns), f32),
            pltpu.VMEM((steps, rows, columns), jnp.bfloat16),
            pltpu.SemaphoreType.DMA((6,)),
        ],
        name="pack",
        compiler_params=LIMIT,
    )(far(model), far(adjoint_last), far(adjoint_late), far(forward))
    model_second = moved(model_second, "depth", second_pairs)
    model_first = moved(model_first, "depth", first_pairs)
    field_second = moved(field_second, "depth", second_pairs)
    field_first = moved(field_first, "depth", first_pairs)
    height = depth_len + 2 * steps + 1
    added = pl.pallas_call(
        functools.partial(injection, steps=steps, depth_len=depth_len, rows=rows),
        in_specs=[SMEM, VMEM, VMEM],
        out_specs=VMEM,
        out_shape=local(steps, height - 2, rows, columns),
        name="injection",
        compiler_params=LIMIT,
    )(far(assignment), far(residuals), far(receiver_cells.transpose(2, 0, 1)))
    joined_rows = own_rows + 2 * part
    joined = pl.pallas_call(
        functools.partial(join_model, layer=channels * share, depth_count=depth_count),
        in_specs=[VMEM] * 3,
        out_specs=VMEM,
        out_shape=local(joined_rows, columns),
        name="join_model",
        compiler_params=LIMIT,
    )(near(own), model_first, model_second)
    swap = lambda array, j: moved(array, "shot", [(i, i ^ j) for i in range(shots)])
    gathered = [near(joined)] + [swap(joined, j) for j in range(1, shots)]
    padded = rows + 2 * PAD
    prepared = pl.pallas_call(
        functools.partial(prepare, steps=steps, depth_count=depth_count),
        in_specs=[VMEM] * 6,
        out_specs=[VMEM] * 5,
        out_shape=[
            local(height, padded, columns),
            local(channels, height - 2, rows, columns),
            local(height - 2, rows, columns),
            local(channels, depth_len + 1, rows, columns),
            local(steps, depth_len + 1, rows, columns),
        ],
        scratch_shapes=[
            pltpu.VMEM((height, padded, columns), f32),
            pltpu.VMEM((height, rows, columns), f32),
            pltpu.VMEM((height, rows, columns), f32),
        ],
        name="prepare",
        compiler_params=LIMIT,
    )(adjoint_last, adjoint_late, forward, field_first, field_second, near(added))
    layers = coarse_len + 2 * reach
    chunk = local(channels * coarse_len * share, columns)
    final, *chunks = pl.pallas_call(
        functools.partial(march, steps=steps, shots=shots, depth_count=depth_count, reach=reach),
        in_specs=[SMEM, SMEM] + [VMEM] * (6 + shots),
        out_specs=[VMEM] * (1 + shots),
        out_shape=[shape(1, depth_len, rows, columns)] + [chunk] * shots,
        scratch_shapes=[
            pltpu.VMEM((shots, joined_rows, columns), f32),
            pltpu.VMEM((layers, channels, rows // 2 + PAD, columns), f32),
            pltpu.VMEM((layers, channels, rows, columns), f32),
            pltpu.VMEM((layers - 1, channels, rows, columns), f32),
            pltpu.VMEM((height, padded, columns), f32),
            pltpu.VMEM((height, padded, columns), f32),
            pltpu.VMEM((height, padded, columns), f32),
            pltpu.VMEM((height, rows, columns), f32),
            pltpu.VMEM((channels, depth_len + 1, rows, columns), f32),
            pltpu.VMEM((4, rows, columns), f32),
        ],
        name="march",
        compiler_params=LIMIT,
    )(
        far(assignment),
        far(source_cells),
        *map(near, prepared),
        near(added),
        *gathered,
    )
    parts = [near(chunks[0])] + [swap(chunks[j], j) for j in range(1, shots)]
    gradients = pl.pallas_call(
        functools.partial(finish, steps=steps),
        in_specs=[VMEM] * shots,
        out_specs=VMEM,
        out_shape=shape(*model.shape),
        name="finish",
        compiler_params=LIMIT,
    )(*parts)
    return final, gradients


def solution(mesh):
    placed = (
        P(None, ("grp", "shot"), "depth", None, None),
        P(("grp", "shot"), "depth", None, None),
        P(("grp", "shot"), "depth", None, None),
        P(("grp", "shot"), None, None),
        P("grp", None),
        P("grp", None, None),
        P("grp"),
        P(None, ("grp", "depth"), "shot", None),
    )
    return jax.shard_map(
        local_part,
        mesh=mesh,
        in_specs=placed,
        out_specs=(
            P(("grp", "shot"), "depth", None, None),
            P(None, ("grp", "depth"), "shot", None),
        ),
        check_vma=False,
    )
```

```python
import functools

import jax
import jax.numpy as jnp
from jax import lax
from jax.experimental import pallas as pl
from jax.experimental.pallas import tpu as pltpu
from jax.sharding import PartitionSpec as P

MUTE = 3
TIME_SQUARED = 0.2
PAD = 8
VMEM = pl.BlockSpec(memory_space=pltpu.VMEM)
SMEM = pl.BlockSpec(memory_space=pltpu.SMEM)
HBM = pl.BlockSpec(memory_space=pltpu.HBM)
LIMIT = pltpu.CompilerParams(vmem_limit_bytes=16 * 1024 * 1024)


def refine_matrix(coarse):
    row = lax.broadcasted_iota(jnp.int32, (coarse, 2 * coarse), 0)
    column = lax.broadcasted_iota(jnp.int32, (coarse, 2 * coarse), 1)
    here = column // 2
    after = jnp.minimum(here + 1, coarse - 1)
    odd = (column % 2) == 1
    at_here = jnp.where(row == here, 1.0, 0.0)
    at_after = jnp.where(row == after, 1.0, 0.0)
    return jnp.where(odd, 0.5 * (at_here + at_after), at_here).astype(jnp.float32)


def exact_dot(left, right, contract=((1,), (0,))):
    right = right.astype(jnp.bfloat16)
    total = None
    for _ in range(3):
        part = left.astype(jnp.bfloat16)
        left = left - part.astype(jnp.float32)
        product = lax.dot_general(
            part, right, (contract, ((), ())), preferred_element_type=jnp.float32
        )
        total = product if total is None else total + product
    return total


def even_depth():
    return lax.axis_index("depth") % 2 == 0


def pack_model(model_ref, own_ref, first_ref, second_ref, *, reach):
    channels, coarse_len, share, coarse_columns = model_ref.shape
    half = channels // 2
    for z in range(coarse_len):
        for k in range(half):
            at = (z * half + k) * share
            own_ref[at : at + share, 0:coarse_columns] = model_ref[k, z]
            own_ref[at : at + share, coarse_columns:] = model_ref[k + half, z]
    part = reach * half * share
    total = coarse_len * half * share
    even = even_depth()

    @pl.when(even)
    def _():
        first_ref[...] = own_ref[total - part : total, :]
        second_ref[...] = own_ref[0:part, :]

    @pl.when(jnp.logical_not(even))
    def _():
        first_ref[...] = own_ref[0:part, :]
        second_ref[...] = own_ref[total - part : total, :]


def pack_fields(
    current_ref, previous_ref, forward_ref, field_first, field_second, weights, sems, *, steps
):
    depth_len = current_ref.shape[1]
    up, down = steps + 1, steps

    def fill(bottom, top):
        copies = [
            pltpu.make_async_copy(forward_ref.at[:, 0, depth_len - 1], weights, sems.at[0]),
            pltpu.make_async_copy(
                current_ref.at[0, depth_len - up : depth_len], bottom.at[0:up], sems.at[1]
            ),
            pltpu.make_async_copy(
                previous_ref.at[0, depth_len - up + 1 : depth_len],
                bottom.at[up : 2 * up - 1],
                sems.at[2],
            ),
            pltpu.make_async_copy(current_ref.at[0, 0:down], top.at[0:down], sems.at[3]),
            pltpu.make_async_copy(
                previous_ref.at[0, 0 : down - 1], top.at[down : 2 * down - 1], sems.at[4]
            ),
        ]
        for copy in copies:
            copy.start()
        copies[0].wait()
        for i in range(steps):
            bottom[2 * up - 1 + i] = weights[i].astype(jnp.float32)
        for copy in copies[1:]:
            copy.wait()

    even = even_depth()

    @pl.when(even)
    def _():
        fill(field_first, field_second)

    @pl.when(jnp.logical_not(even))
    def _():
        fill(field_second, field_first)


def join_model(own_ref, first_ref, second_ref, out_ref, *, layer, depth_count):
    part = first_ref.shape[0]
    own = own_ref.shape[0]
    out_ref[part : part + own, :] = own_ref[...]
    even = even_depth()
    last = lax.axis_index("depth") == depth_count - 1

    @pl.when(even)
    def _():
        out_ref[0:part, :] = second_ref[...]
        out_ref[part + own : 2 * part + own, :] = first_ref[...]

    @pl.when(jnp.logical_not(even))
    def _():
        out_ref[0:part, :] = first_ref[...]
        out_ref[part + own : 2 * part + own, :] = second_ref[...]

    @pl.when(last)
    def _():
        out_ref[part + own : part + own + layer, :] = own_ref[own - layer : own, :]


def injection(assign_ref, residual_ref, receiver_ref, out_ref, *, steps, depth_len, rows):
    receivers = receiver_ref.shape[2]
    columns = out_ref.shape[3]
    count = out_ref.shape[1]
    geometry = assign_ref[lax.axis_index("shot")]
    first = lax.axis_index("depth") * depth_len - steps
    depth = receiver_ref[0, pl.ds(geometry, 1), :] - first
    flat = depth * rows + receiver_ref[1, pl.ds(geometry, 1), :]
    flat = jnp.where((depth >= 0) & (depth < count), flat, -1)
    cells = lax.broadcasted_iota(jnp.int32, (count * rows, receivers), 0)
    one_hot = jnp.where(cells == flat, 1.0, 0.0).astype(jnp.bfloat16)
    lanes = lax.broadcasted_iota(jnp.int32, (columns, receivers), 0)
    here = lanes == receiver_ref[2, pl.ds(geometry, 1), :]
    for i in range(steps):
        left = residual_ref[0, i : i + 1, :]
        total = None
        for _ in range(3):
            rounded = left.astype(jnp.bfloat16).astype(jnp.float32)
            left = left - rounded
            values = jnp.where(here, rounded, 0.0).astype(jnp.bfloat16)
            product = lax.dot_general(
                one_hot, values, (((1,), (1,)), ((), ())), preferred_element_type=jnp.float32
            )
            total = product if total is None else total + product
        out_ref[i] = total.reshape(count, rows, columns)


def slopes_at(field, across, bend, e, rows):
    inner = slice(PAD, PAD + rows)
    before = slice(PAD - 1, PAD - 1 + rows)
    after = slice(PAD + 1, PAD + 1 + rows)
    twice = 2.0 * field[e, inner, :]
    slopes = [
        field[e + 1, inner, :] - twice + field[e - 1, inner, :],
        field[e, after, :] - twice + field[e, before, :],
        bend[e],
        (field[e + 1, after, :] - field[e + 1, before, :])
        - (field[e - 1, after, :] - field[e - 1, before, :]),
        across[e + 1, inner, :] - across[e - 1, inner, :],
        across[e, after, :] - across[e, before, :],
    ]
    return twice, slopes


def columns_of(field, across, bend, lowest, highest, rows):
    columns = field.shape[2]
    inner = slice(PAD, PAD + rows)
    lane = lax.broadcasted_iota(jnp.int32, (rows, columns), 1)
    for e in range(lowest, highest + 1):
        value = field[e, inner, :]
        right = jnp.where(lane == columns - 1, 0.0, pltpu.roll(value, columns - 1, 1))
        left = jnp.where(lane == 0, 0.0, pltpu.roll(value, 1, 1))
        across[e, inner, :] = right - left
        bend[e] = right + left - 2.0 * value


def clear_rim(field, rows):
    height, _, columns = field.shape
    rim = jnp.zeros((height, PAD, columns), jnp.float32)
    field[:, 0:PAD, :] = rim
    field[:, PAD + rows : 2 * PAD + rows, :] = rim


def prepare(
    current_ref,
    previous_ref,
    forward_ref,
    first_ref,
    second_ref,
    added_ref,
    field,
    start_slopes,
    start_base,
    start_totals,
    weights,
    across,
    bend,
    older,
    *,
    steps,
    depth_count,
):
    depth_len, rows, _ = current_ref.shape[1:]
    up, down = steps + 1, steps
    height = up + depth_len + down
    depth_index = lax.axis_index("depth")
    is_even = depth_index % 2 == 0
    inner = slice(PAD, PAD + rows)
    clear_rim(field, rows)
    clear_rim(across, rows)
    field[up : up + depth_len, inner, :] = current_ref[0]
    older[up : up + depth_len] = previous_ref[0]
    for i in range(steps):
        weights[i, 1 : depth_len + 1] = forward_ref[i, 0].astype(jnp.float32)

    def from_above(ref):
        field[0:up, inner, :] = ref[0:up]
        older[1:up] = ref[up : 2 * up - 1]
        for i in range(steps):
            weights[i, 0] = ref[2 * up - 1 + i]

    def from_below(ref):
        field[up + depth_len : height, inner, :] = ref[0:down]
        older[up + depth_len : height - 1] = ref[down : 2 * down - 1]

    @pl.when(is_even)
    def _():
        from_above(second_ref)
        from_below(first_ref)

    @pl.when(jnp.logical_not(is_even))
    def _():
        from_above(first_ref)
        from_below(second_ref)

    @pl.when(depth_index == 0)
    def _():
        field[0:up, inner, :] = jnp.zeros((up,) + current_ref.shape[2:], jnp.float32)
        older[0:up] = jnp.zeros((up,) + current_ref.shape[2:], jnp.float32)

    @pl.when(depth_index == depth_count - 1)
    def _():
        field[up + depth_len : height, inner, :] = jnp.zeros(
            (down,) + current_ref.shape[2:], jnp.float32
        )
        older[up + depth_len : height] = jnp.zeros((down,) + current_ref.shape[2:], jnp.float32)

    columns_of(field, across, bend, 0, height - 1, rows)
    for e in range(1, height - 1):
        twice, slopes = slopes_at(field, across, bend, e, rows)
        for k, slope in enumerate(slopes):
            start_slopes[k, e - 1] = slope
            if up - 1 <= e < up + depth_len:
                start_totals[k, e - up + 1] = weights[0, e - up + 1] * slope
        start_base[e - 1] = twice - older[e] + added_ref[0, e - 1]


def march(
    assign_ref,
    source_ref,
    field,
    start_slopes,
    start_base,
    start_totals,
    weights,
    added_ref,
    *refs,
    steps,
    shots,
    depth_count,
    reach,
):
    gathered = refs[:shots]
    final_ref = refs[shots]
    chunks = refs[shots + 1 : 2 * shots + 1]
    blocks, packed, coarse, even_rows, odd_rows, ones, twos, across, bend, totals, result = refs[
        2 * shots + 1 :
    ]
    depth_len, rows, columns = final_ref.shape[1:]
    channels = start_slopes.shape[0]
    up, down = steps + 1, steps
    height = up + depth_len + down
    depth_index = lax.axis_index("depth")
    shot_index = lax.axis_index("shot")
    is_top = depth_index == 0
    is_last = depth_index == depth_count - 1
    coarse_rows = rows // 2
    share = coarse_rows // shots
    layers = depth_len // 2 + 2 * reach
    inner = slice(PAD, PAD + rows)
    for scratch in (ones, twos, across):
        clear_rim(scratch, rows)

    half = channels // 2
    refine = refine_matrix(columns // 2)
    none = jnp.zeros_like(refine)
    refine_pair = jnp.concatenate(
        [jnp.concatenate([refine, none], axis=1), jnp.concatenate([none, refine], axis=1)], axis=0
    )
    for j in range(shots):
        wide = exact_dot(gathered[j][...], refine_pair)
        start = (shot_index ^ j) * share
        for z in range(layers):
            for k in range(half):
                at = (z * half + k) * share
                for side in range(2):
                    coarse[z, k + side * half, pl.ds(start, share), :] = wide[
                        at : at + share, side * columns : (side + 1) * columns
                    ]
    for z in range(layers):
        for k in range(channels):
            coarse[z, k, coarse_rows : coarse_rows + 1, :] = coarse[
                z, k, coarse_rows - 1 : coarse_rows, :
            ]
            scale = TIME_SQUARED if k < 3 else 0.25 * TIME_SQUARED
            here = coarse[z, k, 0:coarse_rows, :]
            after = coarse[z, k, 1 : coarse_rows + 1, :]
            even_rows[z, k, pl.ds(0, coarse_rows, stride=2), :] = here * scale
            even_rows[z, k, pl.ds(1, coarse_rows, stride=2), :] = (here + after) * (0.5 * scale)
    for z in range(layers - 1):
        for k in range(channels):
            odd_rows[z, k] = (even_rows[z, k] + even_rows[z + 1, k]) * 0.5

    for i in range(steps):
        now = field if i == 0 else (ones if i % 2 else twos)
        old = field if i == 1 else (twos if i % 2 else ones)
        new = twos if i % 2 else ones
        if i > 0:
            columns_of(now, across, bend, i, height - 1 - i, rows)
        for e in range(i + 1, height - 1 - i):
            counted = up - 1 <= e < up + depth_len and i > 0
            stepped = i < steps - 1 or up <= e < up + depth_len
            if not (counted or stepped):
                continue
            if i == 0:
                slopes = [start_slopes[k, e - 1] for k in range(channels)]
                base = start_base[e - 1]
            else:
                twice, slopes = slopes_at(now, across, bend, e, rows)
            if counted:
                weight = weights[i, e - up + 1]
                for k in range(channels):
                    so_far = start_totals if i == 1 else totals
                    totals[k, e - up + 1] = so_far[k, e - up + 1] + weight * slopes[k]
            if stepped:
                if i > 0:
                    base = twice - old[e, inner, :] + added_ref[i, e - 1]
                z = e - up + 2 * reach
                table = even_rows if z % 2 == 0 else odd_rows
                change = table[z // 2, 0] * slopes[0]
                for k in range(1, channels):
                    change = change + table[z // 2, k] * slopes[k]
                updated = base + change
                if e < up:
                    updated = jnp.where(is_top, 0.0, updated)
                if e >= up + depth_len:
                    updated = jnp.where(is_last, 0.0, updated)
                if i < steps - 1:
                    new[e, inner, :] = updated
                else:
                    final_ref[0, e - up] = updated
    if steps == 1:
        totals[...] = start_totals[...]

    geometry = assign_ref[shot_index]
    first = depth_index * depth_len
    row = lax.broadcasted_iota(jnp.int32, (rows, columns), 0)
    lane = lax.broadcasted_iota(jnp.int32, (rows, columns), 1)
    near = (jnp.abs(row - source_ref[geometry, 1]) <= MUTE) & (
        jnp.abs(lane - source_ref[geometry, 2]) <= MUTE
    )
    near = jnp.where(near, 1, 0)
    masks = []
    for e in range(depth_len + 1):
        close = jnp.abs(first + e - 1 - source_ref[geometry, 0]) <= MUTE
        masks.append(near * jnp.where(close, 1, 0) > 0)
    rim_scale = jnp.where(is_top, 0.0, 0.5)
    last_scale = jnp.where(is_last, 1.0, 0.5)
    depth_half = depth_len // 2
    line = lax.broadcasted_iota(jnp.int32, (coarse_rows, columns), 0)
    for k in range(channels):
        kept = [jnp.where(masks[e], 0.0, totals[k, e]) for e in range(depth_len + 1)]
        for z in range(depth_half):
            above = kept[0] * rim_scale if z == 0 else kept[2 * z] * 0.5
            below = kept[2 * z + 2] * (last_scale if z == depth_half - 1 else 0.5)
            slot = (k * depth_half + z) % result.shape[0]
            result[slot] = kept[2 * z + 1] + above + below
            even = result[slot, pl.ds(0, coarse_rows, stride=2), :]
            odd = 0.5 * result[slot, pl.ds(1, coarse_rows, stride=2), :]
            ones[slot, PAD : PAD + coarse_rows, :] = odd
            tail = jnp.where(line == coarse_rows - 1, odd, 0.0)
            value = even + odd + ones[slot, PAD - 1 : PAD - 1 + coarse_rows, :] + tail
            at = (k * depth_half + z) * coarse_rows
            blocks[at : at + coarse_rows, :] = value
    rows_half = half * depth_half * coarse_rows
    gather_rows = lambda low: jnp.concatenate([refine, none] if low else [none, 0.25 * refine], axis=0)
    packed[...] = exact_dot(blocks[0:rows_half, :], gather_rows(True), ((1,), (1,))) + exact_dot(
        blocks[rows_half : 2 * rows_half, :], gather_rows(False), ((1,), (1,))
    )
    for j in range(shots):
        start = (shot_index ^ j) * share
        for layer in range(half * depth_half):
            chunks[j][layer * share : (layer + 1) * share, :] = packed[
                pl.ds(layer * coarse_rows + start, share), :
            ]


def finish(*refs, steps):
    parts, out_ref = refs[:-1], refs[-1]
    channels, depth_len, share, columns = out_ref.shape
    total = parts[0][...]
    for part in parts[1:]:
        total = total + part[...]
    total = total / steps
    half = channels // 2
    for k in range(half):
        for z in range(depth_len):
            at = (k * depth_len + z) * share
            out_ref[k, z] = total[at : at + share, 0:columns]
            out_ref[k + half, z] = total[at : at + share, columns:]


def local_part(
    forward, adjoint_last, adjoint_late, residuals, source_cells, receiver_cells, assignment, model
):
    steps = forward.shape[0]
    shots_here, depth_len, rows, columns = adjoint_last.shape
    channels, coarse_len, share, coarse_columns = model.shape
    shots = lax.axis_size("shot")
    depth_count = lax.axis_size("depth")
    reach = (steps + 1) // 2
    assert shots_here == 1 and depth_count % 2 == 0 and shots & (shots - 1) == 0
    assert channels == 6 and 2 * coarse_columns == columns
    assert depth_len > steps and coarse_len >= reach and share * shots * 2 == rows
    f32 = jnp.float32
    shape = lambda *dims: jax.ShapeDtypeStruct(dims, f32)
    local = lambda *dims: pltpu.VMEM(dims, f32)
    near = lambda array: pltpu.with_memory_space_constraint(array, pltpu.VMEM)
    far = lambda array: pltpu.with_memory_space_constraint(array, pltpu.HBM)
    first_pairs = [(i, i ^ 1) for i in range(depth_count)]
    second_pairs = [(i, (i + 1 if i % 2 else i - 1) % depth_count) for i in range(depth_count)]

    def moved(array, axis, pairs):
        return near(lax.ppermute(array, axis, pairs))

    half = channels // 2
    part = reach * half * share
    own_rows = coarse_len * half * share
    halo = 3 * steps + 1
    own, model_first, model_second = pl.pallas_call(
        functools.partial(pack_model, reach=reach),
        in_specs=[VMEM],
        out_specs=[VMEM] * 3,
        out_shape=[local(own_rows, columns), local(part, columns), local(part, columns)],
        name="pack_model",
        compiler_params=LIMIT,
    )(far(model))
    model_second = moved(model_second, "depth", second_pairs)
    model_first = moved(model_first, "depth", first_pairs)
    field_first, field_second = pl.pallas_call(
        functools.partial(pack_fields, steps=steps),
        in_specs=[HBM] * 3,
        out_specs=[VMEM] * 2,
        out_shape=[local(halo, rows, columns)] * 2,
        scratch_shapes=[
            pltpu.VMEM((steps, rows, columns), jnp.bfloat16),
            pltpu.SemaphoreType.DMA((5,)),
        ],
        name="pack_fields",
        compiler_params=LIMIT,
    )(far(adjoint_last), far(adjoint_late), far(forward))
    field_second = moved(field_second, "depth", second_pairs)
    field_first = moved(field_first, "depth", first_pairs)
    height = depth_len + 2 * steps + 1
    added = pl.pallas_call(
        functools.partial(injection, steps=steps, depth_len=depth_len, rows=rows),
        in_specs=[SMEM, VMEM, VMEM],
        out_specs=VMEM,
        out_shape=local(steps, height - 2, rows, columns),
        name="injection",
        compiler_params=LIMIT,
    )(far(assignment), far(residuals), far(receiver_cells.transpose(2, 0, 1)))
    joined_rows = own_rows + 2 * part
    joined = pl.pallas_call(
        functools.partial(join_model, layer=half * share, depth_count=depth_count),
        in_specs=[VMEM] * 3,
        out_specs=VMEM,
        out_shape=local(joined_rows, columns),
        name="join_model",
        compiler_params=LIMIT,
    )(near(own), model_first, model_second)
    swap = lambda array, j: moved(array, "shot", [(i, i ^ j) for i in range(shots)])
    gathered = [near(joined)] + [swap(joined, j) for j in range(1, shots)]
    padded = rows + 2 * PAD
    prepared = pl.pallas_call(
        functools.partial(prepare, steps=steps, depth_count=depth_count),
        in_specs=[VMEM] * 6,
        out_specs=[VMEM] * 5,
        out_shape=[
            local(height, padded, columns),
            local(channels, height - 2, rows, columns),
            local(height - 2, rows, columns),
            local(channels, depth_len + 1, rows, columns),
            local(steps, depth_len + 1, rows, columns),
        ],
        scratch_shapes=[
            pltpu.VMEM((height, padded, columns), f32),
            pltpu.VMEM((height, rows, columns), f32),
            pltpu.VMEM((height, rows, columns), f32),
        ],
        name="prepare",
        compiler_params=LIMIT,
    )(adjoint_last, adjoint_late, forward, field_first, field_second, near(added))
    layers = coarse_len + 2 * reach
    chunk = local(half * coarse_len * share, columns)
    final, *chunks = pl.pallas_call(
        functools.partial(march, steps=steps, shots=shots, depth_count=depth_count, reach=reach),
        in_specs=[SMEM, SMEM] + [VMEM] * (6 + shots),
        out_specs=[VMEM] * (1 + shots),
        out_shape=[shape(1, depth_len, rows, columns)] + [chunk] * shots,
        scratch_shapes=[
            pltpu.VMEM((channels * coarse_len * rows // 2, columns), f32),
            pltpu.VMEM((half * coarse_len * rows // 2, columns), f32),
            pltpu.VMEM((layers, channels, rows // 2 + PAD, columns), f32),
            pltpu.VMEM((layers, channels, rows, columns), f32),
            pltpu.VMEM((layers - 1, channels, rows, columns), f32),
            pltpu.VMEM((height, padded, columns), f32),
            pltpu.VMEM((height, padded, columns), f32),
            pltpu.VMEM((height, padded, columns), f32),
            pltpu.VMEM((height, rows, columns), f32),
            pltpu.VMEM((channels, depth_len + 1, rows, columns), f32),
            pltpu.VMEM((4, rows, columns), f32),
        ],
        name="march",
        compiler_params=LIMIT,
    )(
        far(assignment),
        far(source_cells),
        *map(near, prepared),
        near(added),
        *gathered,
    )
    parts = [near(chunks[0])] + [swap(chunks[j], j) for j in range(1, shots)]
    gradients = pl.pallas_call(
        functools.partial(finish, steps=steps),
        in_specs=[VMEM] * shots,
        out_specs=VMEM,
        out_shape=shape(*model.shape),
        name="finish",
        compiler_params=LIMIT,
    )(*parts)
    return final, gradients


def solution(mesh):
    placed = (
        P(None, ("grp", "shot"), "depth", None, None),
        P(("grp", "shot"), "depth", None, None),
        P(("grp", "shot"), "depth", None, None),
        P(("grp", "shot"), None, None),
        P("grp", None),
        P("grp", None, None),
        P("grp"),
        P(None, ("grp", "depth"), "shot", None),
    )
    return jax.shard_map(
        local_part,
        mesh=mesh,
        in_specs=placed,
        out_specs=(
            P(("grp", "shot"), "depth", None, None),
            P(None, ("grp", "depth"), "shot", None),
        ),
        check_vma=False,
    )
```

```python
import functools

import jax
import jax.numpy as jnp
from jax import lax
from jax.experimental import pallas as pl
from jax.experimental.pallas import tpu as pltpu
from jax.sharding import PartitionSpec as P

MUTE = 3
TIME_SQUARED = 0.2
PAD = 8
VMEM = pl.BlockSpec(memory_space=pltpu.VMEM)
SMEM = pl.BlockSpec(memory_space=pltpu.SMEM)
HBM = pl.BlockSpec(memory_space=pltpu.HBM)
LIMIT = pltpu.CompilerParams(vmem_limit_bytes=16 * 1024 * 1024)


def refine_matrix(coarse):
    row = lax.broadcasted_iota(jnp.int32, (coarse, 2 * coarse), 0)
    column = lax.broadcasted_iota(jnp.int32, (coarse, 2 * coarse), 1)
    here = column // 2
    after = jnp.minimum(here + 1, coarse - 1)
    odd = (column % 2) == 1
    at_here = jnp.where(row == here, 1.0, 0.0)
    at_after = jnp.where(row == after, 1.0, 0.0)
    return jnp.where(odd, 0.5 * (at_here + at_after), at_here).astype(jnp.float32)


def exact_dot(left, right):
    right = right.astype(jnp.bfloat16)
    parts = []
    for _ in range(3):
        parts.append(left.astype(jnp.bfloat16))
        left = left - parts[-1].astype(jnp.float32)
    product = functools.partial(jnp.dot, preferred_element_type=jnp.float32)
    stacked = jnp.concatenate([right, right], axis=0)
    return product(jnp.concatenate(parts[:2], axis=1), stacked) + product(parts[2], right)


def even_depth():
    return lax.axis_index("depth") % 2 == 0


def pack_model(model_ref, own_ref, first_ref, second_ref, *, reach):
    channels, coarse_len, share, coarse_columns = model_ref.shape
    half = channels // 2
    for z in range(coarse_len):
        for k in range(half):
            at = (z * half + k) * share
            own_ref[at : at + share, 0:coarse_columns] = model_ref[k, z]
            own_ref[at : at + share, coarse_columns:] = model_ref[k + half, z]
    part = reach * half * share
    total = coarse_len * half * share
    even = even_depth()

    @pl.when(even)
    def _():
        first_ref[...] = own_ref[total - part : total, :]
        second_ref[...] = own_ref[0:part, :]

    @pl.when(jnp.logical_not(even))
    def _():
        first_ref[...] = own_ref[0:part, :]
        second_ref[...] = own_ref[total - part : total, :]


def pack_fields(
    current_ref, previous_ref, forward_ref, field_first, field_second, weights, sems, *, steps
):
    depth_len = current_ref.shape[1]
    up, down = steps + 1, steps

    def fill(bottom, top):
        copies = [
            pltpu.make_async_copy(forward_ref.at[:, 0, depth_len - 1], weights, sems.at[0]),
            pltpu.make_async_copy(
                current_ref.at[0, depth_len - up : depth_len], bottom.at[0:up], sems.at[1]
            ),
            pltpu.make_async_copy(
                previous_ref.at[0, depth_len - up + 1 : depth_len],
                bottom.at[up : 2 * up - 1],
                sems.at[2],
            ),
            pltpu.make_async_copy(current_ref.at[0, 0:down], top.at[0:down], sems.at[3]),
            pltpu.make_async_copy(
                previous_ref.at[0, 0 : down - 1], top.at[down : 2 * down - 1], sems.at[4]
            ),
        ]
        for copy in copies:
            copy.start()
        copies[0].wait()
        for i in range(steps):
            bottom[2 * up - 1 + i] = weights[i].astype(jnp.float32)
        for copy in copies[1:]:
            copy.wait()

    even = even_depth()

    @pl.when(even)
    def _():
        fill(field_first, field_second)

    @pl.when(jnp.logical_not(even))
    def _():
        fill(field_second, field_first)


def join_model(own_ref, first_ref, second_ref, out_ref, *, layer, depth_count):
    part = first_ref.shape[0]
    own = own_ref.shape[0]
    out_ref[part : part + own, :] = own_ref[...]
    even = even_depth()
    last = lax.axis_index("depth") == depth_count - 1

    @pl.when(even)
    def _():
        out_ref[0:part, :] = second_ref[...]
        out_ref[part + own : 2 * part + own, :] = first_ref[...]

    @pl.when(jnp.logical_not(even))
    def _():
        out_ref[0:part, :] = first_ref[...]
        out_ref[part + own : 2 * part + own, :] = second_ref[...]

    @pl.when(last)
    def _():
        out_ref[part + own : part + own + layer, :] = own_ref[own - layer : own, :]


def injection(
    assign_ref,
    source_ref,
    residual_ref,
    receiver_ref,
    current_ref,
    previous_ref,
    forward_ref,
    out_ref,
    keep_ref,
    current_out,
    previous_out,
    forward_out,
    sems,
    *,
    steps,
    depth_len,
    rows,
    depth_count,
):
    loads = [
        pltpu.make_async_copy(source, target, sems.at[n])
        for n, (source, target) in enumerate(
            [
                (current_ref, current_out),
                (previous_ref, previous_out),
                (forward_ref, forward_out),
            ]
        )
    ]
    for load in loads:
        load.start()
    receivers = receiver_ref.shape[2]
    columns = out_ref.shape[3]
    count = out_ref.shape[1]
    geometry = assign_ref[lax.axis_index("shot")]
    first = lax.axis_index("depth") * depth_len - steps
    depth = receiver_ref[0, pl.ds(geometry, 1), :] - first
    flat = depth * rows + receiver_ref[1, pl.ds(geometry, 1), :]
    flat = jnp.where((depth >= 0) & (depth < count), flat, -1)
    cells = lax.broadcasted_iota(jnp.int32, (count * rows, receivers), 0)
    one_hot = jnp.where(cells == flat, 1.0, 0.0).astype(jnp.bfloat16)
    lanes = lax.broadcasted_iota(jnp.int32, (columns, receivers), 0)
    here = lanes == receiver_ref[2, pl.ds(geometry, 1), :]
    for i in range(steps):
        left = residual_ref[0, i : i + 1, :]
        total = None
        for _ in range(3):
            rounded = left.astype(jnp.bfloat16).astype(jnp.float32)
            left = left - rounded
            values = jnp.where(here, rounded, 0.0).astype(jnp.bfloat16)
            product = lax.dot_general(
                one_hot, values, (((1,), (1,)), ((), ())), preferred_element_type=jnp.float32
            )
            total = product if total is None else total + product
        out_ref[i] = total.reshape(count, rows, columns)

    depth_index = lax.axis_index("depth")
    row = lax.broadcasted_iota(jnp.int32, (rows, columns), 0)
    lane = lax.broadcasted_iota(jnp.int32, (rows, columns), 1)
    near = (jnp.abs(row - source_ref[geometry, 1]) <= MUTE) & (
        jnp.abs(lane - source_ref[geometry, 2]) <= MUTE
    )
    away = jnp.where(near, 0.0, 1.0)
    for e in range(depth_len + 1):
        close = jnp.abs(depth_index * depth_len + e - 1 - source_ref[geometry, 0]) <= MUTE
        if e == 0:
            scale = jnp.where(depth_index == 0, 0.0, 0.5)
        elif e == depth_len:
            scale = jnp.where(depth_index == depth_count - 1, 1.0, 0.5)
        else:
            scale = 1.0 if e % 2 else 0.5
        keep_ref[e] = jnp.where(close, away, 1.0) * scale
    for load in loads:
        load.wait()


def slopes_at(field, across, bend, e, rows):
    inner = slice(PAD, PAD + rows)
    before = slice(PAD - 1, PAD - 1 + rows)
    after = slice(PAD + 1, PAD + 1 + rows)
    twice = 2.0 * field[e, inner, :]
    slopes = [
        field[e + 1, inner, :] - twice + field[e - 1, inner, :],
        field[e, after, :] - twice + field[e, before, :],
        bend[e],
        (field[e + 1, after, :] - field[e + 1, before, :])
        - (field[e - 1, after, :] - field[e - 1, before, :]),
        across[e + 1, inner, :] - across[e - 1, inner, :],
        across[e, after, :] - across[e, before, :],
    ]
    return twice, slopes


def columns_of(field, across, bend, lowest, highest, rows):
    columns = field.shape[2]
    inner = slice(PAD, PAD + rows)
    lane = lax.broadcasted_iota(jnp.int32, (rows, columns), 1)
    for e in range(lowest, highest + 1):
        value = field[e, inner, :]
        right = jnp.where(lane == columns - 1, 0.0, pltpu.roll(value, columns - 1, 1))
        left = jnp.where(lane == 0, 0.0, pltpu.roll(value, 1, 1))
        across[e, inner, :] = right - left
        bend[e] = right + left - 2.0 * value


def clear_rim(field, rows):
    height, _, columns = field.shape
    rim = jnp.zeros((height, PAD, columns), jnp.float32)
    field[:, 0:PAD, :] = rim
    field[:, PAD + rows : 2 * PAD + rows, :] = rim


def prepare(
    current_ref,
    previous_ref,
    forward_ref,
    first_ref,
    second_ref,
    added_ref,
    keep_ref,
    field,
    start_slopes,
    start_base,
    start_totals,
    weights,
    across,
    bend,
    older,
    *,
    steps,
    depth_count,
):
    depth_len, rows, _ = current_ref.shape[1:]
    up, down = steps + 1, steps
    height = up + depth_len + down
    depth_index = lax.axis_index("depth")
    is_even = depth_index % 2 == 0
    inner = slice(PAD, PAD + rows)
    clear_rim(field, rows)
    clear_rim(across, rows)
    field[up : up + depth_len, inner, :] = current_ref[0]
    older[up : up + depth_len] = previous_ref[0]
    for i in range(steps):
        weights[i, 1 : depth_len + 1] = (
            forward_ref[i, 0].astype(jnp.float32) * keep_ref[1 : depth_len + 1]
        )

    def from_above(ref):
        field[0:up, inner, :] = ref[0:up]
        older[1:up] = ref[up : 2 * up - 1]
        for i in range(steps):
            weights[i, 0] = ref[2 * up - 1 + i] * keep_ref[0]

    def from_below(ref):
        field[up + depth_len : height, inner, :] = ref[0:down]
        older[up + depth_len : height - 1] = ref[down : 2 * down - 1]

    @pl.when(is_even)
    def _():
        from_above(second_ref)
        from_below(first_ref)

    @pl.when(jnp.logical_not(is_even))
    def _():
        from_above(first_ref)
        from_below(second_ref)

    @pl.when(depth_index == 0)
    def _():
        field[0:up, inner, :] = jnp.zeros((up,) + current_ref.shape[2:], jnp.float32)
        older[0:up] = jnp.zeros((up,) + current_ref.shape[2:], jnp.float32)

    @pl.when(depth_index == depth_count - 1)
    def _():
        field[up + depth_len : height, inner, :] = jnp.zeros(
            (down,) + current_ref.shape[2:], jnp.float32
        )
        older[up + depth_len : height] = jnp.zeros((down,) + current_ref.shape[2:], jnp.float32)

    columns_of(field, across, bend, 0, height - 1, rows)
    for e in range(1, height - 1):
        twice, slopes = slopes_at(field, across, bend, e, rows)
        for k, slope in enumerate(slopes):
            start_slopes[k, e - 1] = slope
            if up - 1 <= e < up + depth_len:
                start_totals[k, e - up + 1] = weights[0, e - up + 1] * slope
        start_base[e - 1] = twice - older[e] + added_ref[0, e - 1]


def march(
    field,
    start_slopes,
    start_base,
    start_totals,
    weights,
    added_ref,
    *refs,
    steps,
    shots,
    depth_count,
    reach,
):
    gathered = refs[:shots]
    final_ref = refs[shots]
    chunks = refs[shots + 1 : 2 * shots + 1]
    blocks, packed, coarse, even_rows, odd_rows, ones, twos, across, bend, totals, result = refs[
        2 * shots + 1 :
    ]
    depth_len, rows, columns = final_ref.shape[1:]
    channels = start_slopes.shape[0]
    up, down = steps + 1, steps
    height = up + depth_len + down
    depth_index = lax.axis_index("depth")
    shot_index = lax.axis_index("shot")
    is_top = depth_index == 0
    is_last = depth_index == depth_count - 1
    coarse_rows = rows // 2
    share = coarse_rows // shots
    layers = depth_len // 2 + 2 * reach
    inner = slice(PAD, PAD + rows)
    for scratch in (ones, twos, across):
        clear_rim(scratch, rows)

    half = channels // 2
    refine = refine_matrix(columns // 2)
    none = jnp.zeros_like(refine)
    refine_pair = jnp.concatenate(
        [jnp.concatenate([refine, none], axis=1), jnp.concatenate([none, refine], axis=1)], axis=0
    )
    for j in range(shots):
        wide = exact_dot(gathered[j][...], refine_pair)
        start = (shot_index ^ j) * share
        for z in range(layers):
            for k in range(half):
                at = (z * half + k) * share
                for side in range(2):
                    coarse[z, k + side * half, pl.ds(start, share), :] = wide[
                        at : at + share, side * columns : (side + 1) * columns
                    ]
    for z in range(layers):
        for k in range(channels):
            coarse[z, k, coarse_rows : coarse_rows + 1, :] = coarse[
                z, k, coarse_rows - 1 : coarse_rows, :
            ]
            scale = TIME_SQUARED if k < 3 else 0.25 * TIME_SQUARED
            here = coarse[z, k, 0:coarse_rows, :]
            after = coarse[z, k, 1 : coarse_rows + 1, :]
            even_rows[z, k, pl.ds(0, coarse_rows, stride=2), :] = here * scale
            even_rows[z, k, pl.ds(1, coarse_rows, stride=2), :] = (here + after) * (0.5 * scale)
    for z in range(layers - 1):
        for k in range(channels):
            odd_rows[z, k] = (even_rows[z, k] + even_rows[z + 1, k]) * 0.5

    for i in range(steps):
        now = field if i == 0 else (ones if i % 2 else twos)
        old = field if i == 1 else (twos if i % 2 else ones)
        new = twos if i % 2 else ones
        if i > 0:
            columns_of(now, across, bend, i, height - 1 - i, rows)
        for e in range(i + 1, height - 1 - i):
            counted = up - 1 <= e < up + depth_len and i > 0
            stepped = i < steps - 1 or up <= e < up + depth_len
            if not (counted or stepped):
                continue
            if i == 0:
                slopes = [start_slopes[k, e - 1] for k in range(channels)]
                base = start_base[e - 1]
            else:
                twice, slopes = slopes_at(now, across, bend, e, rows)
            if counted:
                weight = weights[i, e - up + 1]
                for k in range(channels):
                    so_far = start_totals if i == 1 else totals
                    totals[k, e - up + 1] = so_far[k, e - up + 1] + weight * slopes[k]
            if stepped:
                if i > 0:
                    base = twice - old[e, inner, :] + added_ref[i, e - 1]
                z = e - up + 2 * reach
                table = even_rows if z % 2 == 0 else odd_rows
                change = table[z // 2, 0] * slopes[0]
                for k in range(1, channels):
                    change = change + table[z // 2, k] * slopes[k]
                updated = base + change
                if e < up:
                    updated = jnp.where(is_top, 0.0, updated)
                if e >= up + depth_len:
                    updated = jnp.where(is_last, 0.0, updated)
                if i < steps - 1:
                    new[e, inner, :] = updated
                else:
                    final_ref[0, e - up] = updated
    if steps == 1:
        totals[...] = start_totals[...]

    depth_half = depth_len // 2
    line = lax.broadcasted_iota(jnp.int32, (coarse_rows, columns), 0)
    for k in range(channels):
        for z in range(depth_half):
            slot = (k * depth_half + z) % result.shape[0]
            result[slot] = totals[k, 2 * z + 1] + totals[k, 2 * z] + totals[k, 2 * z + 2]
            even = result[slot, pl.ds(0, coarse_rows, stride=2), :]
            odd = 0.5 * result[slot, pl.ds(1, coarse_rows, stride=2), :]
            ones[slot, PAD : PAD + coarse_rows, :] = odd
            tail = jnp.where(line == coarse_rows - 1, odd, 0.0)
            value = even + odd + ones[slot, PAD - 1 : PAD - 1 + coarse_rows, :] + tail
            at = (k * depth_half + z) * coarse_rows
            blocks[at : at + coarse_rows, :] = value
    rows_half = half * depth_half * coarse_rows
    gather = refine.T
    none = jnp.zeros_like(gather)
    packed[...] = exact_dot(
        blocks[0:rows_half, :], jnp.concatenate([gather, none], axis=1)
    ) + exact_dot(
        blocks[rows_half : 2 * rows_half, :], jnp.concatenate([none, 0.25 * gather], axis=1)
    )
    for j in range(shots):
        start = (shot_index ^ j) * share
        for layer in range(half * depth_half):
            chunks[j][layer * share : (layer + 1) * share, :] = packed[
                pl.ds(layer * coarse_rows + start, share), :
            ]


def finish(*refs, steps):
    parts, out_ref = refs[:-1], refs[-1]
    channels, depth_len, share, columns = out_ref.shape
    total = parts[0][...]
    for part in parts[1:]:
        total = total + part[...]
    total = total / steps
    half = channels // 2
    for k in range(half):
        for z in range(depth_len):
            at = (k * depth_len + z) * share
            out_ref[k, z] = total[at : at + share, 0:columns]
            out_ref[k + half, z] = total[at : at + share, columns:]


def local_part(
    forward, adjoint_last, adjoint_late, residuals, source_cells, receiver_cells, assignment, model
):
    steps = forward.shape[0]
    shots_here, depth_len, rows, columns = adjoint_last.shape
    channels, coarse_len, share, coarse_columns = model.shape
    shots = lax.axis_size("shot")
    depth_count = lax.axis_size("depth")
    reach = (steps + 1) // 2
    assert shots_here == 1 and depth_count % 2 == 0 and shots & (shots - 1) == 0
    assert channels == 6 and 2 * coarse_columns == columns
    assert depth_len > steps and coarse_len >= reach and share * shots * 2 == rows
    f32 = jnp.float32
    shape = lambda *dims: jax.ShapeDtypeStruct(dims, f32)
    local = lambda *dims: pltpu.VMEM(dims, f32)
    near = lambda array: pltpu.with_memory_space_constraint(array, pltpu.VMEM)
    far = lambda array: pltpu.with_memory_space_constraint(array, pltpu.HBM)
    first_pairs = [(i, i ^ 1) for i in range(depth_count)]
    second_pairs = [(i, (i + 1 if i % 2 else i - 1) % depth_count) for i in range(depth_count)]

    def moved(array, axis, pairs):
        return near(lax.ppermute(array, axis, pairs))

    half = channels // 2
    part = reach * half * share
    own_rows = coarse_len * half * share
    halo = 3 * steps + 1
    own, model_first, model_second = pl.pallas_call(
        functools.partial(pack_model, reach=reach),
        in_specs=[VMEM],
        out_specs=[VMEM] * 3,
        out_shape=[local(own_rows, columns), local(part, columns), local(part, columns)],
        name="pack_model",
        compiler_params=LIMIT,
    )(far(model))
    model_second = moved(model_second, "depth", second_pairs)
    model_first = moved(model_first, "depth", first_pairs)
    field_first, field_second = pl.pallas_call(
        functools.partial(pack_fields, steps=steps),
        in_specs=[HBM] * 3,
        out_specs=[VMEM] * 2,
        out_shape=[local(halo, rows, columns)] * 2,
        scratch_shapes=[
            pltpu.VMEM((steps, rows, columns), jnp.bfloat16),
            pltpu.SemaphoreType.DMA((5,)),
        ],
        name="pack_fields",
        compiler_params=LIMIT,
    )(far(adjoint_last), far(adjoint_late), far(forward))
    field_second = moved(field_second, "depth", second_pairs)
    field_first = moved(field_first, "depth", first_pairs)
    height = depth_len + 2 * steps + 1
    added, keep, *loaded = pl.pallas_call(
        functools.partial(
            injection, steps=steps, depth_len=depth_len, rows=rows, depth_count=depth_count
        ),
        in_specs=[SMEM, SMEM, VMEM, VMEM, HBM, HBM, HBM],
        out_specs=[VMEM] * 5,
        out_shape=[
            local(steps, height - 2, rows, columns),
            local(depth_len + 1, rows, columns),
            local(1, depth_len, rows, columns),
            local(1, depth_len, rows, columns),
            pltpu.VMEM(forward.shape, forward.dtype),
        ],
        scratch_shapes=[pltpu.SemaphoreType.DMA((3,))],
        name="injection",
        compiler_params=LIMIT,
    )(
        far(assignment),
        far(source_cells),
        far(residuals),
        far(receiver_cells.transpose(2, 0, 1)),
        far(adjoint_last),
        far(adjoint_late),
        far(forward),
    )
    joined_rows = own_rows + 2 * part
    joined = pl.pallas_call(
        functools.partial(join_model, layer=half * share, depth_count=depth_count),
        in_specs=[VMEM] * 3,
        out_specs=VMEM,
        out_shape=local(joined_rows, columns),
        name="join_model",
        compiler_params=LIMIT,
    )(near(own), model_first, model_second)
    swap = lambda array, j: moved(array, "shot", [(i, i ^ j) for i in range(shots)])
    gathered = [near(joined)] + [swap(joined, j) for j in range(1, shots)]
    padded = rows + 2 * PAD
    prepared = pl.pallas_call(
        functools.partial(prepare, steps=steps, depth_count=depth_count),
        in_specs=[VMEM] * 7,
        out_specs=[VMEM] * 5,
        out_shape=[
            local(height, padded, columns),
            local(channels, height - 2, rows, columns),
            local(height - 2, rows, columns),
            local(channels, depth_len + 1, rows, columns),
            local(steps, depth_len + 1, rows, columns),
        ],
        scratch_shapes=[
            pltpu.VMEM((height, padded, columns), f32),
            pltpu.VMEM((height, rows, columns), f32),
            pltpu.VMEM((height, rows, columns), f32),
        ],
        name="prepare",
        compiler_params=LIMIT,
    )(
        *map(near, loaded),
        field_first,
        field_second,
        near(added),
        near(keep),
    )
    layers = coarse_len + 2 * reach
    chunk = local(half * coarse_len * share, columns)
    final, *chunks = pl.pallas_call(
        functools.partial(march, steps=steps, shots=shots, depth_count=depth_count, reach=reach),
        in_specs=[VMEM] * (6 + shots),
        out_specs=[VMEM] * (1 + shots),
        out_shape=[local(1, depth_len, rows, columns)] + [chunk] * shots,
        scratch_shapes=[
            pltpu.VMEM((channels * coarse_len * rows // 2, columns), f32),
            pltpu.VMEM((half * coarse_len * rows // 2, columns), f32),
            pltpu.VMEM((layers, channels, rows // 2 + PAD, columns), f32),
            pltpu.VMEM((layers, channels, rows, columns), f32),
            pltpu.VMEM((layers - 1, channels, rows, columns), f32),
            pltpu.VMEM((height, padded, columns), f32),
            pltpu.VMEM((height, padded, columns), f32),
            pltpu.VMEM((height, padded, columns), f32),
            pltpu.VMEM((height, rows, columns), f32),
            pltpu.VMEM((channels, depth_len + 1, rows, columns), f32),
            pltpu.VMEM((4, rows, columns), f32),
        ],
        name="march",
        compiler_params=LIMIT,
    )(
        *map(near, prepared),
        near(added),
        *gathered,
    )
    parts = [near(chunks[0])] + [swap(chunks[j], j) for j in range(1, shots)]
    gradients = pl.pallas_call(
        functools.partial(finish, steps=steps),
        in_specs=[VMEM] * shots,
        out_specs=VMEM,
        out_shape=shape(*model.shape),
        name="finish",
        compiler_params=LIMIT,
    )(*parts)
    return final, gradients


def solution(mesh):
    placed = (
        P(None, ("grp", "shot"), "depth", None, None),
        P(("grp", "shot"), "depth", None, None),
        P(("grp", "shot"), "depth", None, None),
        P(("grp", "shot"), None, None),
        P("grp", None),
        P("grp", None, None),
        P("grp"),
        P(None, ("grp", "depth"), "shot", None),
    )
    return jax.shard_map(
        local_part,
        mesh=mesh,
        in_specs=placed,
        out_specs=(
            P(("grp", "shot"), "depth", None, None),
            P(None, ("grp", "depth"), "shot", None),
        ),
        check_vma=False,
    )
```

```python
import functools

import jax
import jax.numpy as jnp
from jax import lax
from jax.experimental import pallas as pl
from jax.experimental.pallas import tpu as pltpu
from jax.sharding import PartitionSpec as P

MUTE = 3
TIME_SQUARED = 0.2
PAD = 8
VMEM = pl.BlockSpec(memory_space=pltpu.VMEM)
SMEM = pl.BlockSpec(memory_space=pltpu.SMEM)
HBM = pl.BlockSpec(memory_space=pltpu.HBM)
LIMIT = pltpu.CompilerParams(vmem_limit_bytes=16 * 1024 * 1024)


def refine_matrix(coarse):
    row = lax.broadcasted_iota(jnp.int32, (coarse, 2 * coarse), 0)
    column = lax.broadcasted_iota(jnp.int32, (coarse, 2 * coarse), 1)
    here = column // 2
    after = jnp.minimum(here + 1, coarse - 1)
    odd = (column % 2) == 1
    at_here = jnp.where(row == here, 1.0, 0.0)
    at_after = jnp.where(row == after, 1.0, 0.0)
    return jnp.where(odd, 0.5 * (at_here + at_after), at_here).astype(jnp.float32)


def exact_dot(left, right):
    right = right.astype(jnp.bfloat16)
    parts = []
    for _ in range(3):
        parts.append(left.astype(jnp.bfloat16))
        left = left - parts[-1].astype(jnp.float32)
    product = functools.partial(jnp.dot, preferred_element_type=jnp.float32)
    if right.shape[0] == 128:
        stacked = jnp.concatenate([right, right], axis=0)
        return product(jnp.concatenate(parts[:2], axis=1), stacked) + product(parts[2], right)
    return product(parts[0], right) + product(parts[1], right) + product(parts[2], right)


def even_depth():
    return lax.axis_index("depth") % 2 == 0


def pack_model(model_ref, own_ref, first_ref, second_ref, *, reach):
    channels, coarse_len, share, coarse_columns = model_ref.shape
    half = channels // 2
    for z in range(coarse_len):
        for k in range(half):
            at = (z * half + k) * share
            own_ref[at : at + share, 0:coarse_columns] = model_ref[k, z]
            own_ref[at : at + share, coarse_columns:] = model_ref[k + half, z]
    part = reach * half * share
    total = coarse_len * half * share
    even = even_depth()

    @pl.when(even)
    def _():
        first_ref[...] = own_ref[total - part : total, :]
        second_ref[...] = own_ref[0:part, :]

    @pl.when(jnp.logical_not(even))
    def _():
        first_ref[...] = own_ref[0:part, :]
        second_ref[...] = own_ref[total - part : total, :]


def pack_fields(
    current_ref, previous_ref, forward_ref, field_first, field_second, weights, sems, *, steps
):
    depth_len = current_ref.shape[1]
    up, down = steps + 1, steps

    def fill(bottom, top):
        copies = [
            pltpu.make_async_copy(forward_ref.at[:, 0, depth_len - 1], weights, sems.at[0]),
            pltpu.make_async_copy(
                current_ref.at[0, depth_len - up : depth_len], bottom.at[0:up], sems.at[1]
            ),
            pltpu.make_async_copy(
                previous_ref.at[0, depth_len - up + 1 : depth_len],
                bottom.at[up : 2 * up - 1],
                sems.at[2],
            ),
            pltpu.make_async_copy(current_ref.at[0, 0:down], top.at[0:down], sems.at[3]),
            pltpu.make_async_copy(
                previous_ref.at[0, 0 : down - 1], top.at[down : 2 * down - 1], sems.at[4]
            ),
        ]
        for copy in copies:
            copy.start()
        copies[0].wait()
        for i in range(steps):
            bottom[2 * up - 1 + i] = weights[i].astype(jnp.float32)
        for copy in copies[1:]:
            copy.wait()

    even = even_depth()

    @pl.when(even)
    def _():
        fill(field_first, field_second)

    @pl.when(jnp.logical_not(even))
    def _():
        fill(field_second, field_first)


def join_model(own_ref, first_ref, second_ref, out_ref, *, layer, depth_count):
    part = first_ref.shape[0]
    own = own_ref.shape[0]
    out_ref[part : part + own, :] = own_ref[...]
    even = even_depth()
    last = lax.axis_index("depth") == depth_count - 1

    @pl.when(even)
    def _():
        out_ref[0:part, :] = second_ref[...]
        out_ref[part + own : 2 * part + own, :] = first_ref[...]

    @pl.when(jnp.logical_not(even))
    def _():
        out_ref[0:part, :] = first_ref[...]
        out_ref[part + own : 2 * part + own, :] = second_ref[...]

    @pl.when(last)
    def _():
        out_ref[part + own : part + own + layer, :] = own_ref[own - layer : own, :]


def injection(
    assign_ref,
    source_ref,
    residual_ref,
    receiver_ref,
    current_ref,
    previous_ref,
    forward_ref,
    out_ref,
    keep_ref,
    current_out,
    previous_out,
    forward_out,
    sems,
    *,
    steps,
    depth_len,
    rows,
    depth_count,
):
    loads = [
        pltpu.make_async_copy(source, target, sems.at[n])
        for n, (source, target) in enumerate(
            [
                (current_ref, current_out),
                (previous_ref, previous_out),
                (forward_ref, forward_out),
            ]
        )
    ]
    for load in loads:
        load.start()
    receivers = receiver_ref.shape[2]
    columns = out_ref.shape[3]
    count = out_ref.shape[1]
    geometry = assign_ref[lax.axis_index("shot")]
    first = lax.axis_index("depth") * depth_len - steps
    depth = receiver_ref[0, pl.ds(geometry, 1), :] - first
    flat = depth * rows + receiver_ref[1, pl.ds(geometry, 1), :]
    flat = jnp.where((depth >= 0) & (depth < count), flat, -1)
    cells = lax.broadcasted_iota(jnp.int32, (count * rows, receivers), 0)
    one_hot = jnp.where(cells == flat, 1.0, 0.0).astype(jnp.bfloat16)
    lanes = lax.broadcasted_iota(jnp.int32, (columns, receivers), 0)
    here = lanes == receiver_ref[2, pl.ds(geometry, 1), :]
    for i in range(steps):
        left = residual_ref[0, i : i + 1, :]
        total = None
        for _ in range(3):
            rounded = left.astype(jnp.bfloat16).astype(jnp.float32)
            left = left - rounded
            values = jnp.where(here, rounded, 0.0).astype(jnp.bfloat16)
            product = lax.dot_general(
                one_hot, values, (((1,), (1,)), ((), ())), preferred_element_type=jnp.float32
            )
            total = product if total is None else total + product
        out_ref[i] = total.reshape(count, rows, columns)

    depth_index = lax.axis_index("depth")
    row = lax.broadcasted_iota(jnp.int32, (rows, columns), 0)
    lane = lax.broadcasted_iota(jnp.int32, (rows, columns), 1)
    near = (jnp.abs(row - source_ref[geometry, 1]) <= MUTE) & (
        jnp.abs(lane - source_ref[geometry, 2]) <= MUTE
    )
    away = jnp.where(near, 0.0, 1.0)
    for e in range(depth_len + 1):
        close = jnp.abs(depth_index * depth_len + e - 1 - source_ref[geometry, 0]) <= MUTE
        if e == 0:
            scale = jnp.where(depth_index == 0, 0.0, 0.5)
        elif e == depth_len:
            scale = jnp.where(depth_index == depth_count - 1, 1.0, 0.5)
        else:
            scale = 1.0 if e % 2 else 0.5
        keep_ref[e] = jnp.where(close, away, 1.0) * scale
    for load in loads:
        load.wait()


def slopes_at(field, lines, e, rows):
    across, bend, slant, bow = lines
    inner = slice(PAD, PAD + rows)
    before = slice(PAD - 1, PAD - 1 + rows)
    after = slice(PAD + 1, PAD + 1 + rows)
    twice = 2.0 * field[e, inner, :]
    slopes = [
        field[e + 1, inner, :] - twice + field[e - 1, inner, :],
        bow[e],
        bend[e],
        slant[e + 1] - slant[e - 1],
        across[e + 1, inner, :] - across[e - 1, inner, :],
        across[e, after, :] - across[e, before, :],
    ]
    return twice, slopes


def differences(field, lines, lowest, highest, rows):
    across, bend, slant, bow = lines
    columns = field.shape[2]
    inner = slice(PAD, PAD + rows)
    lane = lax.broadcasted_iota(jnp.int32, (rows, columns), 1)
    for e in range(lowest, highest + 1):
        value = field[e, inner, :]
        twice = 2.0 * value
        right = jnp.where(lane == columns - 1, 0.0, pltpu.roll(value, columns - 1, 1))
        left = jnp.where(lane == 0, 0.0, pltpu.roll(value, 1, 1))
        across[e, inner, :] = right - left
        bend[e] = right + left - twice
        before = field[e, PAD - 1 : PAD - 1 + rows, :]
        after = field[e, PAD + 1 : PAD + 1 + rows, :]
        slant[e] = after - before
        if lowest < e < highest:
            bow[e] = after + before - twice


def clear_rim(field, rows):
    height, _, columns = field.shape
    rim = jnp.zeros((height, PAD, columns), jnp.float32)
    field[:, 0:PAD, :] = rim
    field[:, PAD + rows : 2 * PAD + rows, :] = rim


def prepare(
    current_ref,
    previous_ref,
    forward_ref,
    first_ref,
    second_ref,
    added_ref,
    keep_ref,
    field,
    start_slopes,
    start_base,
    start_totals,
    weights,
    across,
    bend,
    slant,
    bow,
    older,
    *,
    steps,
    depth_count,
):
    depth_len, rows, _ = current_ref.shape[1:]
    up, down = steps + 1, steps
    height = up + depth_len + down
    depth_index = lax.axis_index("depth")
    is_even = depth_index % 2 == 0
    inner = slice(PAD, PAD + rows)
    clear_rim(field, rows)
    clear_rim(across, rows)
    field[up : up + depth_len, inner, :] = current_ref[0]
    older[up : up + depth_len] = previous_ref[0]
    for i in range(steps):
        weights[i, 1 : depth_len + 1] = (
            forward_ref[i, 0].astype(jnp.float32) * keep_ref[1 : depth_len + 1]
        )

    def from_above(ref):
        field[0:up, inner, :] = ref[0:up]
        older[1:up] = ref[up : 2 * up - 1]
        for i in range(steps):
            weights[i, 0] = ref[2 * up - 1 + i] * keep_ref[0]

    def from_below(ref):
        field[up + depth_len : height, inner, :] = ref[0:down]
        older[up + depth_len : height - 1] = ref[down : 2 * down - 1]

    @pl.when(is_even)
    def _():
        from_above(second_ref)
        from_below(first_ref)

    @pl.when(jnp.logical_not(is_even))
    def _():
        from_above(first_ref)
        from_below(second_ref)

    @pl.when(depth_index == 0)
    def _():
        field[0:up, inner, :] = jnp.zeros((up,) + current_ref.shape[2:], jnp.float32)
        older[0:up] = jnp.zeros((up,) + current_ref.shape[2:], jnp.float32)

    @pl.when(depth_index == depth_count - 1)
    def _():
        field[up + depth_len : height, inner, :] = jnp.zeros(
            (down,) + current_ref.shape[2:], jnp.float32
        )
        older[up + depth_len : height] = jnp.zeros((down,) + current_ref.shape[2:], jnp.float32)

    lines = (across, bend, slant, bow)
    differences(field, lines, 0, height - 1, rows)
    for e in range(1, height - 1):
        twice, slopes = slopes_at(field, lines, e, rows)
        for k, slope in enumerate(slopes):
            start_slopes[k, e - 1] = slope
            if up - 1 <= e < up + depth_len:
                start_totals[k, e - up + 1] = weights[0, e - up + 1] * slope
        start_base[e - 1] = twice - older[e] + added_ref[0, e - 1]


def change_at(even_rows, odd_rows, slopes, z):
    table = even_rows if z % 2 == 0 else odd_rows
    change = table[z // 2, 0] * slopes[0]
    for k in range(1, len(slopes)):
        change = change + table[z // 2, k] * slopes[k]
    return change


def last_update(*refs, steps, reach):
    now, old, even_rows, odd_rows, added_ref, final_ref, *lines = refs
    depth_len, rows, _ = final_ref.shape[1:]
    up = steps + 1
    clear_rim(lines[0], rows)
    differences(now, lines, up - 1, up + depth_len, rows)
    for e in range(up, up + depth_len):
        twice, slopes = slopes_at(now, lines, e, rows)
        base = twice - old[e, PAD : PAD + rows, :] + added_ref[steps - 1, e - 1]
        final_ref[0, e - up] = base + change_at(even_rows, odd_rows, slopes, e - up + 2 * reach)


def march(
    field,
    start_slopes,
    start_base,
    start_totals,
    weights,
    added_ref,
    *refs,
    steps,
    shots,
    depth_count,
    reach,
):
    gathered, chunks = refs[:shots], refs[shots : 2 * shots]
    ones, twos, even_rows, odd_rows, blocks, packed, coarse, *lines, totals, result = refs[
        2 * shots :
    ]
    across = lines[0]
    rows, columns = start_base.shape[1:]
    channels, depth_len = start_slopes.shape[0], weights.shape[1] - 1
    up, down = steps + 1, steps
    height = up + depth_len + down
    depth_index = lax.axis_index("depth")
    shot_index = lax.axis_index("shot")
    is_top = depth_index == 0
    is_last = depth_index == depth_count - 1
    coarse_rows = rows // 2
    share = coarse_rows // shots
    layers = depth_len // 2 + 2 * reach
    inner = slice(PAD, PAD + rows)
    for scratch in (ones, twos, across):
        clear_rim(scratch, rows)

    half = channels // 2
    refine = refine_matrix(columns // 2)
    none = jnp.zeros_like(refine)
    refine_pair = jnp.concatenate(
        [jnp.concatenate([refine, none], axis=1), jnp.concatenate([none, refine], axis=1)], axis=0
    )
    for j in range(shots):
        wide = exact_dot(gathered[j][...], refine_pair)
        start = (shot_index ^ j) * share
        for z in range(layers):
            for k in range(half):
                at = (z * half + k) * share
                for side in range(2):
                    coarse[z, k + side * half, pl.ds(start, share), :] = wide[
                        at : at + share, side * columns : (side + 1) * columns
                    ]
    for z in range(layers):
        for k in range(channels):
            coarse[z, k, coarse_rows : coarse_rows + 1, :] = coarse[
                z, k, coarse_rows - 1 : coarse_rows, :
            ]
            scale = TIME_SQUARED if k < 3 else 0.25 * TIME_SQUARED
            here = coarse[z, k, 0:coarse_rows, :]
            after = coarse[z, k, 1 : coarse_rows + 1, :]
            even_rows[z, k, pl.ds(0, coarse_rows, stride=2), :] = here * scale
            even_rows[z, k, pl.ds(1, coarse_rows, stride=2), :] = (here + after) * (0.5 * scale)
    for z in range(layers - 1):
        for k in range(channels):
            odd_rows[z, k] = (even_rows[z, k] + even_rows[z + 1, k]) * 0.5

    for i in range(steps):
        now = field if i == 0 else (ones if i % 2 else twos)
        old = field if i == 1 else (twos if i % 2 else ones)
        new = twos if i % 2 else ones
        last = i == steps - 1
        if i > 0:
            differences(now, lines, i, height - 1 - i, rows)
        for e in range(i + 1, height - 1 - i):
            counted = up - 1 <= e < up + depth_len and i > 0
            if last and not counted:
                continue
            if i == 0:
                slopes = [start_slopes[k, e - 1] for k in range(channels)]
                base = start_base[e - 1]
            else:
                twice, slopes = slopes_at(now, lines, e, rows)
            if counted:
                weight = weights[i, e - up + 1]
                for k in range(channels):
                    so_far = start_totals if i == 1 else totals
                    totals[k, e - up + 1] = so_far[k, e - up + 1] + weight * slopes[k]
            if not last:
                if i > 0:
                    base = twice - old[e, inner, :] + added_ref[i, e - 1]
                updated = base + change_at(even_rows, odd_rows, slopes, e - up + 2 * reach)
                if e < up:
                    updated = jnp.where(is_top, 0.0, updated)
                if e >= up + depth_len:
                    updated = jnp.where(is_last, 0.0, updated)
                new[e, inner, :] = updated

    gather = refine.T
    none = jnp.zeros_like(gather)
    gather_pair = jnp.concatenate(
        [
            jnp.concatenate([gather, none], axis=1),
            jnp.concatenate([none, 0.25 * gather], axis=1),
        ],
        axis=0,
    )
    depth_half = depth_len // 2
    line = lax.broadcasted_iota(jnp.int32, (coarse_rows, columns), 0)
    for z in range(depth_half):
        for channel in range(channels):
            slot = (z * channels + channel) % result.shape[0]
            result[slot] = (
                totals[channel, 2 * z + 1] + totals[channel, 2 * z] + totals[channel, 2 * z + 2]
            )
            even = result[slot, pl.ds(0, coarse_rows, stride=2), :]
            odd = 0.5 * result[slot, pl.ds(1, coarse_rows, stride=2), :]
            across[slot, PAD : PAD + coarse_rows, :] = odd
            tail = jnp.where(line == coarse_rows - 1, odd, 0.0)
            value = even + odd + across[slot, PAD - 1 : PAD - 1 + coarse_rows, :] + tail
            at, side = (channel % half) * coarse_rows, channel // half * columns
            blocks[z, at : at + coarse_rows, side : side + columns] = value
        packed[z] = exact_dot(blocks[z], gather_pair)
    for j in range(shots):
        start = (shot_index ^ j) * share
        for k in range(half):
            for z in range(depth_half):
                at = (k * depth_half + z) * share
                chunks[j][at : at + share, :] = packed[z, pl.ds(k * coarse_rows + start, share), :]


def finish(*refs, steps):
    parts, out_ref = refs[:-1], refs[-1]
    channels, depth_len, share, columns = out_ref.shape
    total = parts[0][...]
    for part in parts[1:]:
        total = total + part[...]
    total = total / steps
    half = channels // 2
    for k in range(half):
        for z in range(depth_len):
            at = (k * depth_len + z) * share
            out_ref[k, z] = total[at : at + share, 0:columns]
            out_ref[k + half, z] = total[at : at + share, columns:]


def local_part(
    forward, adjoint_last, adjoint_late, residuals, source_cells, receiver_cells, assignment, model
):
    steps = forward.shape[0]
    shots_here, depth_len, rows, columns = adjoint_last.shape
    channels, coarse_len, share, coarse_columns = model.shape
    shots = lax.axis_size("shot")
    depth_count = lax.axis_size("depth")
    reach = (steps + 1) // 2
    assert shots_here == 1 and depth_count % 2 == 0 and shots & (shots - 1) == 0
    assert channels == 6 and 2 * coarse_columns == columns
    assert steps % 2 == 0 and steps > 2 and depth_len > steps and coarse_len >= reach and share * shots * 2 == rows
    f32 = jnp.float32
    shape = lambda *dims: jax.ShapeDtypeStruct(dims, f32)
    local = lambda *dims: pltpu.VMEM(dims, f32)
    near = lambda array: pltpu.with_memory_space_constraint(array, pltpu.VMEM)
    far = lambda array: pltpu.with_memory_space_constraint(array, pltpu.HBM)
    first_pairs = [(i, i ^ 1) for i in range(depth_count)]
    second_pairs = [(i, (i + 1 if i % 2 else i - 1) % depth_count) for i in range(depth_count)]

    def moved(array, axis, pairs):
        return near(lax.ppermute(array, axis, pairs))

    half = channels // 2
    part = reach * half * share
    own_rows = coarse_len * half * share
    halo = 3 * steps + 1
    own, model_first, model_second = pl.pallas_call(
        functools.partial(pack_model, reach=reach),
        in_specs=[VMEM],
        out_specs=[VMEM] * 3,
        out_shape=[local(own_rows, columns), local(part, columns), local(part, columns)],
        name="pack_model",
        compiler_params=LIMIT,
    )(far(model))
    model_second = moved(model_second, "depth", second_pairs)
    model_first = moved(model_first, "depth", first_pairs)
    field_first, field_second = pl.pallas_call(
        functools.partial(pack_fields, steps=steps),
        in_specs=[HBM] * 3,
        out_specs=[VMEM] * 2,
        out_shape=[local(halo, rows, columns)] * 2,
        scratch_shapes=[
            pltpu.VMEM((steps, rows, columns), jnp.bfloat16),
            pltpu.SemaphoreType.DMA((5,)),
        ],
        name="pack_fields",
        compiler_params=LIMIT,
    )(far(adjoint_last), far(adjoint_late), far(forward))
    field_second = moved(field_second, "depth", second_pairs)
    field_first = moved(field_first, "depth", first_pairs)
    height = depth_len + 2 * steps + 1
    added, keep, *loaded = pl.pallas_call(
        functools.partial(
            injection, steps=steps, depth_len=depth_len, rows=rows, depth_count=depth_count
        ),
        in_specs=[SMEM, SMEM, VMEM, VMEM, HBM, HBM, HBM],
        out_specs=[VMEM] * 5,
        out_shape=[
            local(steps, height - 2, rows, columns),
            local(depth_len + 1, rows, columns),
            local(1, depth_len, rows, columns),
            local(1, depth_len, rows, columns),
            pltpu.VMEM(forward.shape, forward.dtype),
        ],
        scratch_shapes=[pltpu.SemaphoreType.DMA((3,))],
        name="injection",
        compiler_params=LIMIT,
    )(
        far(assignment),
        far(source_cells),
        far(residuals),
        far(receiver_cells.transpose(2, 0, 1)),
        far(adjoint_last),
        far(adjoint_late),
        far(forward),
    )
    joined_rows = own_rows + 2 * part
    joined = pl.pallas_call(
        functools.partial(join_model, layer=half * share, depth_count=depth_count),
        in_specs=[VMEM] * 3,
        out_specs=VMEM,
        out_shape=local(joined_rows, columns),
        name="join_model",
        compiler_params=LIMIT,
    )(near(own), model_first, model_second)
    swap = lambda array, j: moved(array, "shot", [(i, i ^ j) for i in range(shots)])
    gathered = [near(joined)] + [swap(joined, j) for j in range(1, shots)]
    padded = rows + 2 * PAD
    prepared = pl.pallas_call(
        functools.partial(prepare, steps=steps, depth_count=depth_count),
        in_specs=[VMEM] * 7,
        out_specs=[VMEM] * 5,
        out_shape=[
            local(height, padded, columns),
            local(channels, height - 2, rows, columns),
            local(height - 2, rows, columns),
            local(channels, depth_len + 1, rows, columns),
            local(steps, depth_len + 1, rows, columns),
        ],
        scratch_shapes=[
            local(height, padded, columns),
            local(height, rows, columns),
            local(height, rows, columns),
            local(height, rows, columns),
            local(height, rows, columns),
        ],
        name="prepare",
        compiler_params=LIMIT,
    )(
        *map(near, loaded),
        field_first,
        field_second,
        near(added),
        near(keep),
    )
    layers = coarse_len + 2 * reach
    chunk = local(half * coarse_len * share, columns)
    lines = [
        local(height, padded, columns),
        local(height, rows, columns),
        local(height, rows, columns),
        local(height, rows, columns),
    ]
    outs = pl.pallas_call(
        functools.partial(march, steps=steps, shots=shots, depth_count=depth_count, reach=reach),
        in_specs=[VMEM] * (6 + shots),
        out_specs=[VMEM] * (shots + 4),
        out_shape=[chunk] * shots
        + [
            local(height, padded, columns),
            local(height, padded, columns),
            local(layers, channels, rows, columns),
            local(layers - 1, channels, rows, columns),
        ],
        scratch_shapes=[
            local(coarse_len, half * rows // 2, 2 * columns),
            local(coarse_len, half * rows // 2, columns),
            local(layers, channels, rows // 2 + PAD, columns),
            *lines,
            local(channels, depth_len + 1, rows, columns),
            local(12, rows, columns),
        ],
        name="march",
        compiler_params=LIMIT,
    )(*map(near, prepared), near(added), *gathered)
    chunks, kept = outs[:shots], outs[shots:]
    final = pl.pallas_call(
        functools.partial(last_update, steps=steps, reach=reach),
        in_specs=[VMEM] * 5,
        out_specs=VMEM,
        out_shape=shape(1, depth_len, rows, columns),
        scratch_shapes=lines,
        name="last_update",
        compiler_params=LIMIT,
    )(*map(near, kept), near(added))
    parts = [near(chunks[0])] + [swap(chunks[j], j) for j in range(1, shots)]
    gradients = pl.pallas_call(
        functools.partial(finish, steps=steps),
        in_specs=[VMEM] * shots,
        out_specs=VMEM,
        out_shape=shape(*model.shape),
        name="finish",
        compiler_params=LIMIT,
    )(*parts)
    return final, gradients


def solution(mesh):
    placed = (
        P(None, ("grp", "shot"), "depth", None, None),
        P(("grp", "shot"), "depth", None, None),
        P(("grp", "shot"), "depth", None, None),
        P(("grp", "shot"), None, None),
        P("grp", None),
        P("grp", None, None),
        P("grp"),
        P(None, ("grp", "depth"), "shot", None),
    )
    return jax.shard_map(
        local_part,
        mesh=mesh,
        in_specs=placed,
        out_specs=(
            P(("grp", "shot"), "depth", None, None),
            P(None, ("grp", "depth"), "shot", None),
        ),
        check_vma=False,
    )
```

```python
import functools

import jax
import jax.numpy as jnp
from jax import lax
from jax.experimental import pallas as pl
from jax.experimental.pallas import tpu as pltpu
from jax.sharding import PartitionSpec as P

MUTE = 3
TIME_SQUARED = 0.2
PAD = 8
VMEM = pl.BlockSpec(memory_space=pltpu.VMEM)
SMEM = pl.BlockSpec(memory_space=pltpu.SMEM)
HBM = pl.BlockSpec(memory_space=pltpu.HBM)
LIMIT = pltpu.CompilerParams(vmem_limit_bytes=16 * 1024 * 1024)


def refine_matrix(coarse):
    row = lax.broadcasted_iota(jnp.int32, (coarse, 2 * coarse), 0)
    column = lax.broadcasted_iota(jnp.int32, (coarse, 2 * coarse), 1)
    here = column // 2
    after = jnp.minimum(here + 1, coarse - 1)
    odd = (column % 2) == 1
    at_here = jnp.where(row == here, 1.0, 0.0)
    at_after = jnp.where(row == after, 1.0, 0.0)
    return jnp.where(odd, 0.5 * (at_here + at_after), at_here).astype(jnp.float32)


def exact_dot(left, right):
    right = right.astype(jnp.bfloat16)
    parts = []
    for _ in range(3):
        parts.append(left.astype(jnp.bfloat16))
        left = left - parts[-1].astype(jnp.float32)
    product = functools.partial(jnp.dot, preferred_element_type=jnp.float32)
    if right.shape[0] == 128:
        stacked = jnp.concatenate([right, right], axis=0)
        return product(jnp.concatenate(parts[:2], axis=1), stacked) + product(parts[2], right)
    return product(parts[0], right) + product(parts[1], right) + product(parts[2], right)


def even_depth():
    return lax.axis_index("depth") % 2 == 0


def pack(
    model_ref,
    current_ref,
    previous_ref,
    forward_ref,
    own_ref,
    model_first,
    model_second,
    field_first,
    field_second,
    block,
    weights,
    sems,
    *,
    steps,
    reach,
):
    channels, coarse_len, share, coarse_columns = model_ref.shape
    half = channels // 2
    depth_len = current_ref.shape[1]
    up, down = steps + 1, steps
    part = reach * half * share
    total = coarse_len * half * share
    model_copy = pltpu.make_async_copy(model_ref, block, sems.at[5])
    model_copy.start()

    def fill(bottom, top, model_bottom, model_top):
        copies = [
            pltpu.make_async_copy(forward_ref.at[:, 0, depth_len - 1], weights, sems.at[0]),
            pltpu.make_async_copy(
                current_ref.at[0, depth_len - up : depth_len], bottom.at[0:up], sems.at[1]
            ),
            pltpu.make_async_copy(
                previous_ref.at[0, depth_len - up + 1 : depth_len],
                bottom.at[up : 2 * up - 1],
                sems.at[2],
            ),
            pltpu.make_async_copy(current_ref.at[0, 0:down], top.at[0:down], sems.at[3]),
            pltpu.make_async_copy(
                previous_ref.at[0, 0 : down - 1], top.at[down : 2 * down - 1], sems.at[4]
            ),
        ]
        for copy in copies:
            copy.start()
        model_copy.wait()
        for z in range(coarse_len):
            for k in range(half):
                at = (z * half + k) * share
                own_ref[at : at + share, 0:coarse_columns] = block[k, z]
                own_ref[at : at + share, coarse_columns:] = block[k + half, z]
        model_bottom[...] = own_ref[total - part : total, :]
        model_top[...] = own_ref[0:part, :]
        copies[0].wait()
        for i in range(steps):
            bottom[2 * up - 1 + i] = weights[i].astype(jnp.float32)
        for copy in copies[1:]:
            copy.wait()

    even = even_depth()

    @pl.when(even)
    def _():
        fill(field_first, field_second, model_first, model_second)

    @pl.when(jnp.logical_not(even))
    def _():
        fill(field_second, field_first, model_second, model_first)


def join_model(own_ref, first_ref, second_ref, out_ref, *, layer, depth_count):
    part = first_ref.shape[0]
    own = own_ref.shape[0]
    out_ref[part : part + own, :] = own_ref[...]
    even = even_depth()
    last = lax.axis_index("depth") == depth_count - 1

    @pl.when(even)
    def _():
        out_ref[0:part, :] = second_ref[...]
        out_ref[part + own : 2 * part + own, :] = first_ref[...]

    @pl.when(jnp.logical_not(even))
    def _():
        out_ref[0:part, :] = first_ref[...]
        out_ref[part + own : 2 * part + own, :] = second_ref[...]

    @pl.when(last)
    def _():
        out_ref[part + own : part + own + layer, :] = own_ref[own - layer : own, :]


def injection(
    assign_hbm,
    source_hbm,
    residual_hbm,
    receiver_hbm,
    current_ref,
    previous_ref,
    forward_ref,
    out_ref,
    keep_ref,
    current_out,
    previous_out,
    forward_out,
    assign_ref,
    source_ref,
    residual_ref,
    receiver_ref,
    sems,
    *,
    steps,
    depth_len,
    rows,
    depth_count,
):
    loads = [
        pltpu.make_async_copy(source, target, sems.at[n])
        for n, (source, target) in enumerate(
            [
                (assign_hbm, assign_ref),
                (source_hbm, source_ref),
                (receiver_hbm, receiver_ref),
                (residual_hbm, residual_ref),
                (current_ref, current_out),
                (previous_ref, previous_out),
                (forward_ref, forward_out),
            ]
        )
    ]
    for load in loads:
        load.start()
    for load in loads[:4]:
        load.wait()
    receivers = receiver_ref.shape[2]
    columns = out_ref.shape[3]
    count = out_ref.shape[1]
    geometry = assign_ref[lax.axis_index("shot")]
    first = lax.axis_index("depth") * depth_len - steps
    depth = receiver_ref[0, pl.ds(geometry, 1), :] - first
    flat = depth * rows + receiver_ref[1, pl.ds(geometry, 1), :]
    flat = jnp.where((depth >= 0) & (depth < count), flat, -1)
    cells = lax.broadcasted_iota(jnp.int32, (count * rows, receivers), 0)
    one_hot = jnp.where(cells == flat, 1.0, 0.0).astype(jnp.bfloat16)
    lanes = lax.broadcasted_iota(jnp.int32, (columns, receivers), 0)
    here = lanes == receiver_ref[2, pl.ds(geometry, 1), :]
    for i in range(steps):
        left = residual_ref[0, i : i + 1, :]
        total = None
        for _ in range(3):
            rounded = left.astype(jnp.bfloat16).astype(jnp.float32)
            left = left - rounded
            values = jnp.where(here, rounded, 0.0).astype(jnp.bfloat16)
            product = lax.dot_general(
                one_hot, values, (((1,), (1,)), ((), ())), preferred_element_type=jnp.float32
            )
            total = product if total is None else total + product
        out_ref[i] = total.reshape(count, rows, columns)

    depth_index = lax.axis_index("depth")
    row = lax.broadcasted_iota(jnp.int32, (rows, columns), 0)
    lane = lax.broadcasted_iota(jnp.int32, (rows, columns), 1)
    near = (jnp.abs(row - source_ref[geometry, 1]) <= MUTE) & (
        jnp.abs(lane - source_ref[geometry, 2]) <= MUTE
    )
    away = jnp.where(near, 0.0, 1.0)
    for e in range(depth_len + 1):
        close = jnp.abs(depth_index * depth_len + e - 1 - source_ref[geometry, 0]) <= MUTE
        if e == 0:
            scale = jnp.where(depth_index == 0, 0.0, 0.5)
        elif e == depth_len:
            scale = jnp.where(depth_index == depth_count - 1, 1.0, 0.5)
        else:
            scale = 1.0 if e % 2 else 0.5
        keep_ref[e] = jnp.where(close, away, 1.0) * scale
    for load in loads[4:]:
        load.wait()


def slopes_at(field, lines, e, rows):
    across, bend, slant, bow = lines
    inner = slice(PAD, PAD + rows)
    before = slice(PAD - 1, PAD - 1 + rows)
    after = slice(PAD + 1, PAD + 1 + rows)
    twice = 2.0 * field[e, inner, :]
    slopes = [
        field[e + 1, inner, :] - twice + field[e - 1, inner, :],
        bow[e],
        bend[e],
        slant[e + 1] - slant[e - 1],
        across[e + 1, inner, :] - across[e - 1, inner, :],
        across[e, after, :] - across[e, before, :],
    ]
    return twice, slopes


def differences(field, lines, lowest, highest, rows):
    across, bend, slant, bow = lines
    columns = field.shape[2]
    inner = slice(PAD, PAD + rows)
    lane = lax.broadcasted_iota(jnp.int32, (rows, columns), 1)
    for e in range(lowest, highest + 1):
        value = field[e, inner, :]
        twice = 2.0 * value
        right = jnp.where(lane == columns - 1, 0.0, pltpu.roll(value, columns - 1, 1))
        left = jnp.where(lane == 0, 0.0, pltpu.roll(value, 1, 1))
        across[e, inner, :] = right - left
        bend[e] = right + left - twice
        before = field[e, PAD - 1 : PAD - 1 + rows, :]
        after = field[e, PAD + 1 : PAD + 1 + rows, :]
        slant[e] = after - before
        if lowest < e < highest:
            bow[e] = after + before - twice


def clear_rim(field, rows):
    height, _, columns = field.shape
    rim = jnp.zeros((height, PAD, columns), jnp.float32)
    field[:, 0:PAD, :] = rim
    field[:, PAD + rows : 2 * PAD + rows, :] = rim


def prepare(
    current_ref,
    previous_ref,
    forward_ref,
    first_ref,
    second_ref,
    added_ref,
    keep_ref,
    field,
    start_slopes,
    start_base,
    start_totals,
    weights,
    across,
    bend,
    slant,
    bow,
    older,
    *,
    steps,
    depth_count,
):
    depth_len, rows, _ = current_ref.shape[1:]
    up, down = steps + 1, steps
    height = up + depth_len + down
    depth_index = lax.axis_index("depth")
    is_even = depth_index % 2 == 0
    inner = slice(PAD, PAD + rows)
    clear_rim(field, rows)
    clear_rim(across, rows)
    field[up : up + depth_len, inner, :] = current_ref[0]
    older[up : up + depth_len] = previous_ref[0]
    for i in range(steps):
        weights[i, 1 : depth_len + 1] = (
            forward_ref[i, 0].astype(jnp.float32) * keep_ref[1 : depth_len + 1]
        )

    def from_above(ref):
        field[0:up, inner, :] = ref[0:up]
        older[1:up] = ref[up : 2 * up - 1]
        for i in range(steps):
            weights[i, 0] = ref[2 * up - 1 + i] * keep_ref[0]

    def from_below(ref):
        field[up + depth_len : height, inner, :] = ref[0:down]
        older[up + depth_len : height - 1] = ref[down : 2 * down - 1]

    @pl.when(is_even)
    def _():
        from_above(second_ref)
        from_below(first_ref)

    @pl.when(jnp.logical_not(is_even))
    def _():
        from_above(first_ref)
        from_below(second_ref)

    @pl.when(depth_index == 0)
    def _():
        field[0:up, inner, :] = jnp.zeros((up,) + current_ref.shape[2:], jnp.float32)
        older[0:up] = jnp.zeros((up,) + current_ref.shape[2:], jnp.float32)

    @pl.when(depth_index == depth_count - 1)
    def _():
        field[up + depth_len : height, inner, :] = jnp.zeros(
            (down,) + current_ref.shape[2:], jnp.float32
        )
        older[up + depth_len : height] = jnp.zeros((down,) + current_ref.shape[2:], jnp.float32)

    lines = (across, bend, slant, bow)
    differences(field, lines, 0, height - 1, rows)
    for e in range(1, height - 1):
        twice, slopes = slopes_at(field, lines, e, rows)
        for k, slope in enumerate(slopes):
            start_slopes[k, e - 1] = slope
            if up - 1 <= e < up + depth_len:
                start_totals[k, e - up + 1] = weights[0, e - up + 1] * slope
        start_base[e - 1] = twice - older[e] + added_ref[0, e - 1]


def change_at(even_rows, odd_rows, slopes, z):
    table = even_rows if z % 2 == 0 else odd_rows
    change = table[z // 2, 0] * slopes[0]
    for k in range(1, len(slopes)):
        change = change + table[z // 2, k] * slopes[k]
    return change


def last_update(*refs, steps, reach):
    now, old, even_rows, odd_rows, added_ref, final_ref, *lines = refs
    depth_len, rows, _ = final_ref.shape[1:]
    up = steps + 1
    clear_rim(lines[0], rows)
    differences(now, lines, up - 1, up + depth_len, rows)
    for e in range(up, up + depth_len):
        twice, slopes = slopes_at(now, lines, e, rows)
        base = twice - old[e, PAD : PAD + rows, :] + added_ref[steps - 1, e - 1]
        final_ref[0, e - up] = base + change_at(even_rows, odd_rows, slopes, e - up + 2 * reach)


def march(
    field,
    start_slopes,
    start_base,
    start_totals,
    weights,
    added_ref,
    *refs,
    steps,
    shots,
    depth_count,
    reach,
):
    gathered, chunks = refs[:shots], refs[shots : 2 * shots]
    ones, twos, even_rows, odd_rows, blocks, packed, coarse, *lines, totals, result = refs[
        2 * shots :
    ]
    across = lines[0]
    rows, columns = start_base.shape[1:]
    channels, depth_len = start_slopes.shape[0], weights.shape[1] - 1
    up, down = steps + 1, steps
    height = up + depth_len + down
    depth_index = lax.axis_index("depth")
    shot_index = lax.axis_index("shot")
    is_top = depth_index == 0
    is_last = depth_index == depth_count - 1
    coarse_rows = rows // 2
    share = coarse_rows // shots
    layers = depth_len // 2 + 2 * reach
    inner = slice(PAD, PAD + rows)
    for scratch in (ones, twos, across):
        clear_rim(scratch, rows)

    half = channels // 2
    refine = refine_matrix(columns // 2)
    none = jnp.zeros_like(refine)
    refine_pair = jnp.concatenate(
        [jnp.concatenate([refine, none], axis=1), jnp.concatenate([none, refine], axis=1)], axis=0
    )
    for j in range(shots):
        wide = exact_dot(gathered[j][...], refine_pair)
        start = (shot_index ^ j) * share
        for z in range(layers):
            for k in range(half):
                at = (z * half + k) * share
                for side in range(2):
                    coarse[z, k + side * half, pl.ds(start, share), :] = wide[
                        at : at + share, side * columns : (side + 1) * columns
                    ]
    for z in range(layers):
        for k in range(channels):
            coarse[z, k, coarse_rows : coarse_rows + 1, :] = coarse[
                z, k, coarse_rows - 1 : coarse_rows, :
            ]
            scale = TIME_SQUARED if k < 3 else 0.25 * TIME_SQUARED
            here = coarse[z, k, 0:coarse_rows, :]
            after = coarse[z, k, 1 : coarse_rows + 1, :]
            even_rows[z, k, pl.ds(0, coarse_rows, stride=2), :] = here * scale
            even_rows[z, k, pl.ds(1, coarse_rows, stride=2), :] = (here + after) * (0.5 * scale)
    for z in range(layers - 1):
        for k in range(channels):
            odd_rows[z, k] = (even_rows[z, k] + even_rows[z + 1, k]) * 0.5

    for i in range(steps):
        now = field if i == 0 else (ones if i % 2 else twos)
        old = field if i == 1 else (twos if i % 2 else ones)
        new = twos if i % 2 else ones
        last = i == steps - 1
        if i > 0:
            differences(now, lines, i, height - 1 - i, rows)
        for e in range(i + 1, height - 1 - i):
            counted = up - 1 <= e < up + depth_len and i > 0
            if last and not counted:
                continue
            if i == 0:
                slopes = [start_slopes[k, e - 1] for k in range(channels)]
                base = start_base[e - 1]
            else:
                twice, slopes = slopes_at(now, lines, e, rows)
            if counted:
                weight = weights[i, e - up + 1]
                for k in range(channels):
                    so_far = start_totals if i == 1 else totals
                    totals[k, e - up + 1] = so_far[k, e - up + 1] + weight * slopes[k]
            if not last:
                if i > 0:
                    base = twice - old[e, inner, :] + added_ref[i, e - 1]
                updated = base + change_at(even_rows, odd_rows, slopes, e - up + 2 * reach)
                if e < up:
                    updated = jnp.where(is_top, 0.0, updated)
                if e >= up + depth_len:
                    updated = jnp.where(is_last, 0.0, updated)
                new[e, inner, :] = updated

    gather = refine.T
    none = jnp.zeros_like(gather)
    gather_pair = jnp.concatenate(
        [
            jnp.concatenate([gather, none], axis=1),
            jnp.concatenate([none, 0.25 * gather], axis=1),
        ],
        axis=0,
    )
    depth_half = depth_len // 2
    line = lax.broadcasted_iota(jnp.int32, (coarse_rows, columns), 0)
    for z in range(depth_half):
        for channel in range(channels):
            slot = (z * channels + channel) % result.shape[0]
            result[slot] = (
                totals[channel, 2 * z + 1] + totals[channel, 2 * z] + totals[channel, 2 * z + 2]
            )
            even = result[slot, pl.ds(0, coarse_rows, stride=2), :]
            odd = 0.5 * result[slot, pl.ds(1, coarse_rows, stride=2), :]
            across[slot, PAD : PAD + coarse_rows, :] = odd
            tail = jnp.where(line == coarse_rows - 1, odd, 0.0)
            value = even + odd + across[slot, PAD - 1 : PAD - 1 + coarse_rows, :] + tail
            at, side = (channel % half) * coarse_rows, channel // half * columns
            blocks[z, at : at + coarse_rows, side : side + columns] = value
        packed[z] = exact_dot(blocks[z], gather_pair)
    for j in range(shots):
        start = (shot_index ^ j) * share
        for k in range(half):
            for z in range(depth_half):
                at = (k * depth_half + z) * share
                chunks[j][at : at + share, :] = packed[z, pl.ds(k * coarse_rows + start, share), :]


def finish(*refs, steps):
    parts, out_ref = refs[:-1], refs[-1]
    channels, depth_len, share, columns = out_ref.shape
    total = parts[0][...]
    for part in parts[1:]:
        total = total + part[...]
    total = total / steps
    half = channels // 2
    for k in range(half):
        for z in range(depth_len):
            at = (k * depth_len + z) * share
            out_ref[k, z] = total[at : at + share, 0:columns]
            out_ref[k + half, z] = total[at : at + share, columns:]


def local_part(
    forward, adjoint_last, adjoint_late, residuals, source_cells, receiver_cells, assignment, model
):
    steps = forward.shape[0]
    shots_here, depth_len, rows, columns = adjoint_last.shape
    channels, coarse_len, share, coarse_columns = model.shape
    shots = lax.axis_size("shot")
    depth_count = lax.axis_size("depth")
    reach = (steps + 1) // 2
    assert shots_here == 1 and depth_count % 2 == 0 and shots & (shots - 1) == 0
    assert channels == 6 and 2 * coarse_columns == columns
    assert steps % 2 == 0 and steps > 2 and depth_len > steps and coarse_len >= reach and share * shots * 2 == rows
    f32 = jnp.float32
    shape = lambda *dims: jax.ShapeDtypeStruct(dims, f32)
    local = lambda *dims: pltpu.VMEM(dims, f32)
    near = lambda array: pltpu.with_memory_space_constraint(array, pltpu.VMEM)
    far = lambda array: pltpu.with_memory_space_constraint(array, pltpu.HBM)
    first_pairs = [(i, i ^ 1) for i in range(depth_count)]
    second_pairs = [(i, (i + 1 if i % 2 else i - 1) % depth_count) for i in range(depth_count)]

    def moved(array, axis, pairs):
        return near(lax.ppermute(array, axis, pairs))

    half = channels // 2
    part = reach * half * share
    own_rows = coarse_len * half * share
    halo = 3 * steps + 1
    own, model_first, model_second, field_first, field_second = pl.pallas_call(
        functools.partial(pack, steps=steps, reach=reach),
        in_specs=[HBM] * 4,
        out_specs=[VMEM] * 5,
        out_shape=[local(own_rows, columns), local(part, columns), local(part, columns)]
        + [local(halo, rows, columns)] * 2,
        scratch_shapes=[
            local(*model.shape),
            pltpu.VMEM((steps, rows, columns), jnp.bfloat16),
            pltpu.SemaphoreType.DMA((6,)),
        ],
        name="pack",
        compiler_params=LIMIT,
    )(far(model), far(adjoint_last), far(adjoint_late), far(forward))
    model_second = moved(model_second, "depth", second_pairs)
    model_first = moved(model_first, "depth", first_pairs)
    field_second = moved(field_second, "depth", second_pairs)
    field_first = moved(field_first, "depth", first_pairs)
    height = depth_len + 2 * steps + 1
    added, keep, *loaded = pl.pallas_call(
        functools.partial(
            injection, steps=steps, depth_len=depth_len, rows=rows, depth_count=depth_count
        ),
        in_specs=[HBM] * 7,
        out_specs=[VMEM] * 5,
        out_shape=[
            local(steps, height - 2, rows, columns),
            local(depth_len + 1, rows, columns),
            local(1, depth_len, rows, columns),
            local(1, depth_len, rows, columns),
            pltpu.VMEM(forward.shape, forward.dtype),
        ],
        scratch_shapes=[
            pltpu.SMEM(assignment.shape, jnp.int32),
            pltpu.SMEM(source_cells.shape, jnp.int32),
            local(*residuals.shape),
            pltpu.VMEM((receiver_cells.shape[2],) + receiver_cells.shape[:2], jnp.int32),
            pltpu.SemaphoreType.DMA((7,)),
        ],
        name="injection",
        compiler_params=LIMIT,
    )(
        far(assignment),
        far(source_cells),
        far(residuals),
        far(receiver_cells.transpose(2, 0, 1)),
        far(adjoint_last),
        far(adjoint_late),
        far(forward),
    )
    joined_rows = own_rows + 2 * part
    joined = pl.pallas_call(
        functools.partial(join_model, layer=half * share, depth_count=depth_count),
        in_specs=[VMEM] * 3,
        out_specs=VMEM,
        out_shape=local(joined_rows, columns),
        name="join_model",
        compiler_params=LIMIT,
    )(near(own), model_first, model_second)
    swap = lambda array, j: moved(array, "shot", [(i, i ^ j) for i in range(shots)])
    gathered = [near(joined)] + [swap(joined, j) for j in range(1, shots)]
    padded = rows + 2 * PAD
    prepared = pl.pallas_call(
        functools.partial(prepare, steps=steps, depth_count=depth_count),
        in_specs=[VMEM] * 7,
        out_specs=[VMEM] * 5,
        out_shape=[
            local(height, padded, columns),
            local(channels, height - 2, rows, columns),
            local(height - 2, rows, columns),
            local(channels, depth_len + 1, rows, columns),
            local(steps, depth_len + 1, rows, columns),
        ],
        scratch_shapes=[
            local(height, padded, columns),
            local(height, rows, columns),
            local(height, rows, columns),
            local(height, rows, columns),
            local(height, rows, columns),
        ],
        name="prepare",
        compiler_params=LIMIT,
    )(
        *map(near, loaded),
        field_first,
        field_second,
        near(added),
        near(keep),
    )
    layers = coarse_len + 2 * reach
    chunk = local(half * coarse_len * share, columns)
    lines = [
        local(height, padded, columns),
        local(height, rows, columns),
        local(height, rows, columns),
        local(height, rows, columns),
    ]
    outs = pl.pallas_call(
        functools.partial(march, steps=steps, shots=shots, depth_count=depth_count, reach=reach),
        in_specs=[VMEM] * (6 + shots),
        out_specs=[VMEM] * (shots + 4),
        out_shape=[chunk] * shots
        + [
            local(height, padded, columns),
            local(height, padded, columns),
            local(layers, channels, rows, columns),
            local(layers - 1, channels, rows, columns),
        ],
        scratch_shapes=[
            local(coarse_len, half * rows // 2, 2 * columns),
            local(coarse_len, half * rows // 2, columns),
            local(layers, channels, rows // 2 + PAD, columns),
            *lines,
            local(channels, depth_len + 1, rows, columns),
            local(12, rows, columns),
        ],
        name="march",
        compiler_params=LIMIT,
    )(*map(near, prepared), near(added), *gathered)
    chunks, kept = outs[:shots], outs[shots:]
    final = pl.pallas_call(
        functools.partial(last_update, steps=steps, reach=reach),
        in_specs=[VMEM] * 5,
        out_specs=VMEM,
        out_shape=shape(1, depth_len, rows, columns),
        scratch_shapes=lines,
        name="last_update",
        compiler_params=LIMIT,
    )(*map(near, kept), near(added))
    parts = [near(chunks[0])] + [swap(chunks[j], j) for j in range(1, shots)]
    gradients = pl.pallas_call(
        functools.partial(finish, steps=steps),
        in_specs=[VMEM] * shots,
        out_specs=VMEM,
        out_shape=shape(*model.shape),
        name="finish",
        compiler_params=LIMIT,
    )(*parts)
    return final, gradients


def solution(mesh):
    placed = (
        P(None, ("grp", "shot"), "depth", None, None),
        P(("grp", "shot"), "depth", None, None),
        P(("grp", "shot"), "depth", None, None),
        P(("grp", "shot"), None, None),
        P("grp", None),
        P("grp", None, None),
        P("grp"),
        P(None, ("grp", "depth"), "shot", None),
    )
    return jax.shard_map(
        local_part,
        mesh=mesh,
        in_specs=placed,
        out_specs=(
            P(("grp", "shot"), "depth", None, None),
            P(None, ("grp", "depth"), "shot", None),
        ),
        check_vma=False,
    )
```

```python
import functools

import jax
import jax.numpy as jnp
from jax import lax
from jax.experimental import pallas as pl
from jax.experimental.pallas import tpu as pltpu
from jax.sharding import PartitionSpec as P

MUTE = 3
TIME_SQUARED = 0.2
PAD = 8
VMEM = pl.BlockSpec(memory_space=pltpu.VMEM)
SMEM = pl.BlockSpec(memory_space=pltpu.SMEM)
HBM = pl.BlockSpec(memory_space=pltpu.HBM)
LIMIT = pltpu.CompilerParams(vmem_limit_bytes=16 * 1024 * 1024)


def refine_matrix(coarse):
    row = lax.broadcasted_iota(jnp.int32, (coarse, 2 * coarse), 0)
    column = lax.broadcasted_iota(jnp.int32, (coarse, 2 * coarse), 1)
    here = column // 2
    after = jnp.minimum(here + 1, coarse - 1)
    odd = (column % 2) == 1
    at_here = jnp.where(row == here, 1.0, 0.0)
    at_after = jnp.where(row == after, 1.0, 0.0)
    return jnp.where(odd, 0.5 * (at_here + at_after), at_here).astype(jnp.float32)


def exact_dot(left, right):
    right = right.astype(jnp.bfloat16)
    parts = []
    for _ in range(3):
        parts.append(left.astype(jnp.bfloat16))
        left = left - parts[-1].astype(jnp.float32)
    product = functools.partial(jnp.dot, preferred_element_type=jnp.float32)
    if right.shape[0] == 128:
        stacked = jnp.concatenate([right, right], axis=0)
        return product(jnp.concatenate(parts[:2], axis=1), stacked) + product(parts[2], right)
    return product(parts[0], right) + product(parts[1], right) + product(parts[2], right)


def pair_matrix(coarse):
    refine = refine_matrix(coarse)
    none = jnp.zeros_like(refine)
    return jnp.concatenate(
        [jnp.concatenate([refine, none], axis=1), jnp.concatenate([none, refine], axis=1)], axis=0
    )


def refine_early(*refs):
    blocks, out_ref = refs[:-1], refs[-1]
    matrix = pair_matrix(blocks[0].shape[1] // 2)
    for j, block in enumerate(blocks):
        out_ref[j] = exact_dot(block[...], matrix)


def even_depth():
    return lax.axis_index("depth") % 2 == 0


def pack(
    model_ref,
    current_ref,
    previous_ref,
    forward_ref,
    own_ref,
    model_first,
    model_second,
    field_first,
    field_second,
    block,
    weights,
    sems,
    *,
    steps,
    reach,
):
    channels, coarse_len, share, coarse_columns = model_ref.shape
    half = channels // 2
    depth_len = current_ref.shape[1]
    up, down = steps + 1, steps
    part = reach * half * share
    total = coarse_len * half * share
    model_copy = pltpu.make_async_copy(model_ref, block, sems.at[5])
    model_copy.start()

    def fill(bottom, top, model_bottom, model_top):
        copies = [
            pltpu.make_async_copy(forward_ref.at[:, 0, depth_len - 1], weights, sems.at[0]),
            pltpu.make_async_copy(
                current_ref.at[0, depth_len - up : depth_len], bottom.at[0:up], sems.at[1]
            ),
            pltpu.make_async_copy(
                previous_ref.at[0, depth_len - up + 1 : depth_len],
                bottom.at[up : 2 * up - 1],
                sems.at[2],
            ),
            pltpu.make_async_copy(current_ref.at[0, 0:down], top.at[0:down], sems.at[3]),
            pltpu.make_async_copy(
                previous_ref.at[0, 0 : down - 1], top.at[down : 2 * down - 1], sems.at[4]
            ),
        ]
        for copy in copies:
            copy.start()
        model_copy.wait()
        for z in range(coarse_len):
            for k in range(half):
                at = (z * half + k) * share
                own_ref[at : at + share, 0:coarse_columns] = block[k, z]
                own_ref[at : at + share, coarse_columns:] = block[k + half, z]
        model_bottom[...] = own_ref[total - part : total, :]
        model_top[...] = own_ref[0:part, :]
        copies[0].wait()
        for i in range(steps):
            bottom[2 * up - 1 + i] = weights[i].astype(jnp.float32)
        for copy in copies[1:]:
            copy.wait()

    even = even_depth()

    @pl.when(even)
    def _():
        fill(field_first, field_second, model_first, model_second)

    @pl.when(jnp.logical_not(even))
    def _():
        fill(field_second, field_first, model_second, model_first)


def join_model(own_ref, first_ref, second_ref, out_ref, *, layer, depth_count):
    part = first_ref.shape[0]
    own = own_ref.shape[0]
    out_ref[part : part + own, :] = own_ref[...]
    even = even_depth()
    last = lax.axis_index("depth") == depth_count - 1

    @pl.when(even)
    def _():
        out_ref[0:part, :] = second_ref[...]
        out_ref[part + own : 2 * part + own, :] = first_ref[...]

    @pl.when(jnp.logical_not(even))
    def _():
        out_ref[0:part, :] = first_ref[...]
        out_ref[part + own : 2 * part + own, :] = second_ref[...]

    @pl.when(last)
    def _():
        out_ref[part + own : part + own + layer, :] = own_ref[own - layer : own, :]


def injection(
    assign_hbm,
    source_hbm,
    residual_hbm,
    receiver_hbm,
    current_ref,
    previous_ref,
    forward_ref,
    out_ref,
    keep_ref,
    current_out,
    previous_out,
    forward_out,
    assign_ref,
    source_ref,
    residual_ref,
    receiver_ref,
    sems,
    *,
    steps,
    depth_len,
    rows,
    depth_count,
):
    loads = [
        pltpu.make_async_copy(source, target, sems.at[n])
        for n, (source, target) in enumerate(
            [
                (assign_hbm, assign_ref),
                (source_hbm, source_ref),
                (receiver_hbm, receiver_ref),
                (residual_hbm, residual_ref),
                (current_ref, current_out),
                (previous_ref, previous_out),
                (forward_ref, forward_out),
            ]
        )
    ]
    for load in loads:
        load.start()
    for load in loads[:4]:
        load.wait()
    receivers = receiver_ref.shape[2]
    columns = out_ref.shape[3]
    count = out_ref.shape[1]
    geometry = assign_ref[lax.axis_index("shot")]
    first = lax.axis_index("depth") * depth_len - steps
    depth = receiver_ref[0, pl.ds(geometry, 1), :] - first
    flat = depth * rows + receiver_ref[1, pl.ds(geometry, 1), :]
    flat = jnp.where((depth >= 0) & (depth < count), flat, -1)
    cells = lax.broadcasted_iota(jnp.int32, (count * rows, receivers), 0)
    one_hot = jnp.where(cells == flat, 1.0, 0.0).astype(jnp.bfloat16)
    lanes = lax.broadcasted_iota(jnp.int32, (columns, receivers), 0)
    here = lanes == receiver_ref[2, pl.ds(geometry, 1), :]
    for i in range(steps):
        left = residual_ref[0, i : i + 1, :]
        total = None
        for _ in range(3):
            rounded = left.astype(jnp.bfloat16).astype(jnp.float32)
            left = left - rounded
            values = jnp.where(here, rounded, 0.0).astype(jnp.bfloat16)
            product = lax.dot_general(
                one_hot, values, (((1,), (1,)), ((), ())), preferred_element_type=jnp.float32
            )
            total = product if total is None else total + product
        out_ref[i] = total.reshape(count, rows, columns)

    depth_index = lax.axis_index("depth")
    row = lax.broadcasted_iota(jnp.int32, (rows, columns), 0)
    lane = lax.broadcasted_iota(jnp.int32, (rows, columns), 1)
    near = (jnp.abs(row - source_ref[geometry, 1]) <= MUTE) & (
        jnp.abs(lane - source_ref[geometry, 2]) <= MUTE
    )
    away = jnp.where(near, 0.0, 1.0)
    for e in range(depth_len + 1):
        close = jnp.abs(depth_index * depth_len + e - 1 - source_ref[geometry, 0]) <= MUTE
        if e == 0:
            scale = jnp.where(depth_index == 0, 0.0, 0.5)
        elif e == depth_len:
            scale = jnp.where(depth_index == depth_count - 1, 1.0, 0.5)
        else:
            scale = 1.0 if e % 2 else 0.5
        keep_ref[e] = jnp.where(close, away, 1.0) * scale
    for load in loads[4:]:
        load.wait()


def slopes_at(field, lines, e, rows):
    across, bend, slant, bow = lines
    inner = slice(PAD, PAD + rows)
    before = slice(PAD - 1, PAD - 1 + rows)
    after = slice(PAD + 1, PAD + 1 + rows)
    twice = 2.0 * field[e, inner, :]
    slopes = [
        field[e + 1, inner, :] - twice + field[e - 1, inner, :],
        bow[e],
        bend[e],
        slant[e + 1] - slant[e - 1],
        across[e + 1, inner, :] - across[e - 1, inner, :],
        across[e, after, :] - across[e, before, :],
    ]
    return twice, slopes


def differences(field, lines, lowest, highest, rows):
    across, bend, slant, bow = lines
    columns = field.shape[2]
    inner = slice(PAD, PAD + rows)
    lane = lax.broadcasted_iota(jnp.int32, (rows, columns), 1)
    for e in range(lowest, highest + 1):
        value = field[e, inner, :]
        twice = 2.0 * value
        right = jnp.where(lane == columns - 1, 0.0, pltpu.roll(value, columns - 1, 1))
        left = jnp.where(lane == 0, 0.0, pltpu.roll(value, 1, 1))
        across[e, inner, :] = right - left
        bend[e] = right + left - twice
        before = field[e, PAD - 1 : PAD - 1 + rows, :]
        after = field[e, PAD + 1 : PAD + 1 + rows, :]
        slant[e] = after - before
        if lowest < e < highest:
            bow[e] = after + before - twice


def clear_rim(field, rows):
    height, _, columns = field.shape
    rim = jnp.zeros((height, PAD, columns), jnp.float32)
    field[:, 0:PAD, :] = rim
    field[:, PAD + rows : 2 * PAD + rows, :] = rim


def prepare(
    current_ref,
    previous_ref,
    forward_ref,
    first_ref,
    second_ref,
    added_ref,
    keep_ref,
    field,
    start_slopes,
    start_base,
    start_totals,
    weights,
    across,
    bend,
    slant,
    bow,
    older,
    *,
    steps,
    depth_count,
):
    depth_len, rows, _ = current_ref.shape[1:]
    up, down = steps + 1, steps
    height = up + depth_len + down
    depth_index = lax.axis_index("depth")
    is_even = depth_index % 2 == 0
    inner = slice(PAD, PAD + rows)
    clear_rim(field, rows)
    clear_rim(across, rows)
    field[up : up + depth_len, inner, :] = current_ref[0]
    older[up : up + depth_len] = previous_ref[0]
    for i in range(steps):
        weights[i, 1 : depth_len + 1] = (
            forward_ref[i, 0].astype(jnp.float32) * keep_ref[1 : depth_len + 1]
        )

    def from_above(ref):
        field[0:up, inner, :] = ref[0:up]
        older[1:up] = ref[up : 2 * up - 1]
        for i in range(steps):
            weights[i, 0] = ref[2 * up - 1 + i] * keep_ref[0]

    def from_below(ref):
        field[up + depth_len : height, inner, :] = ref[0:down]
        older[up + depth_len : height - 1] = ref[down : 2 * down - 1]

    @pl.when(is_even)
    def _():
        from_above(second_ref)
        from_below(first_ref)

    @pl.when(jnp.logical_not(is_even))
    def _():
        from_above(first_ref)
        from_below(second_ref)

    @pl.when(depth_index == 0)
    def _():
        field[0:up, inner, :] = jnp.zeros((up,) + current_ref.shape[2:], jnp.float32)
        older[0:up] = jnp.zeros((up,) + current_ref.shape[2:], jnp.float32)

    @pl.when(depth_index == depth_count - 1)
    def _():
        field[up + depth_len : height, inner, :] = jnp.zeros(
            (down,) + current_ref.shape[2:], jnp.float32
        )
        older[up + depth_len : height] = jnp.zeros((down,) + current_ref.shape[2:], jnp.float32)

    lines = (across, bend, slant, bow)
    differences(field, lines, 0, height - 1, rows)
    for e in range(1, height - 1):
        twice, slopes = slopes_at(field, lines, e, rows)
        for k, slope in enumerate(slopes):
            start_slopes[k, e - 1] = slope
            if up - 1 <= e < up + depth_len:
                start_totals[k, e - up + 1] = weights[0, e - up + 1] * slope
        start_base[e - 1] = twice - older[e] + added_ref[0, e - 1]


def change_at(even_rows, odd_rows, slopes, z):
    table = even_rows if z % 2 == 0 else odd_rows
    change = table[z // 2, 0] * slopes[0]
    for k in range(1, len(slopes)):
        change = change + table[z // 2, k] * slopes[k]
    return change


def last_update(*refs, steps, reach):
    now, old, even_rows, odd_rows, added_ref, final_ref, *lines = refs
    depth_len, rows, _ = final_ref.shape[1:]
    up = steps + 1
    clear_rim(lines[0], rows)
    differences(now, lines, up - 1, up + depth_len, rows)
    for e in range(up, up + depth_len):
        twice, slopes = slopes_at(now, lines, e, rows)
        base = twice - old[e, PAD : PAD + rows, :] + added_ref[steps - 1, e - 1]
        final_ref[0, e - up] = base + change_at(even_rows, odd_rows, slopes, e - up + 2 * reach)


def march(
    field,
    start_slopes,
    start_base,
    start_totals,
    weights,
    added_ref,
    *refs,
    steps,
    shots,
    depth_count,
    reach,
):
    early_ref, *refs = refs
    late, refs = refs[:2], refs[2:]
    chunks = refs[:shots]
    ones, twos, even_rows, odd_rows, blocks, packed, coarse, *lines, totals, result = refs[
        shots:
    ]
    across = lines[0]
    rows, columns = start_base.shape[1:]
    channels, depth_len = start_slopes.shape[0], weights.shape[1] - 1
    up, down = steps + 1, steps
    height = up + depth_len + down
    depth_index = lax.axis_index("depth")
    shot_index = lax.axis_index("shot")
    is_top = depth_index == 0
    is_last = depth_index == depth_count - 1
    coarse_rows = rows // 2
    share = coarse_rows // shots
    layers = depth_len // 2 + 2 * reach
    inner = slice(PAD, PAD + rows)
    for scratch in (ones, twos, across):
        clear_rim(scratch, rows)

    half = channels // 2
    refine = refine_matrix(columns // 2)
    count = late[0].shape[0]
    both = exact_dot(
        jnp.concatenate([ref[...] for ref in late], axis=0), pair_matrix(columns // 2)
    )
    for j in range(shots):
        if j in (1, 2):
            wide = both[(j - 1) * count : j * count]
        else:
            wide = early_ref[max(j - 2, 0)]
        start = (shot_index ^ j) * share
        for z in range(layers):
            for k in range(half):
                at = (z * half + k) * share
                for side in range(2):
                    coarse[z, k + side * half, pl.ds(start, share), :] = wide[
                        at : at + share, side * columns : (side + 1) * columns
                    ]
    for z in range(layers):
        for k in range(channels):
            coarse[z, k, coarse_rows : coarse_rows + 1, :] = coarse[
                z, k, coarse_rows - 1 : coarse_rows, :
            ]
            scale = TIME_SQUARED if k < 3 else 0.25 * TIME_SQUARED
            here = coarse[z, k, 0:coarse_rows, :]
            after = coarse[z, k, 1 : coarse_rows + 1, :]
            even_rows[z, k, pl.ds(0, coarse_rows, stride=2), :] = here * scale
            even_rows[z, k, pl.ds(1, coarse_rows, stride=2), :] = (here + after) * (0.5 * scale)
    for z in range(layers - 1):
        for k in range(channels):
            odd_rows[z, k] = (even_rows[z, k] + even_rows[z + 1, k]) * 0.5

    for i in range(steps):
        now = field if i == 0 else (ones if i % 2 else twos)
        old = field if i == 1 else (twos if i % 2 else ones)
        new = twos if i % 2 else ones
        last = i == steps - 1
        if i > 0:
            differences(now, lines, i, height - 1 - i, rows)
        for e in range(i + 1, height - 1 - i):
            counted = up - 1 <= e < up + depth_len and i > 0
            if last and not counted:
                continue
            if i == 0:
                slopes = [start_slopes[k, e - 1] for k in range(channels)]
                base = start_base[e - 1]
            else:
                twice, slopes = slopes_at(now, lines, e, rows)
            if counted:
                weight = weights[i, e - up + 1]
                for k in range(channels):
                    so_far = start_totals if i == 1 else totals
                    totals[k, e - up + 1] = so_far[k, e - up + 1] + weight * slopes[k]
            if not last:
                if i > 0:
                    base = twice - old[e, inner, :] + added_ref[i, e - 1]
                updated = base + change_at(even_rows, odd_rows, slopes, e - up + 2 * reach)
                if e < up:
                    updated = jnp.where(is_top, 0.0, updated)
                if e >= up + depth_len:
                    updated = jnp.where(is_last, 0.0, updated)
                new[e, inner, :] = updated

    gather = refine.T
    none = jnp.zeros_like(gather)
    gather_pair = jnp.concatenate(
        [
            jnp.concatenate([gather, none], axis=1),
            jnp.concatenate([none, 0.25 * gather], axis=1),
        ],
        axis=0,
    )
    depth_half = depth_len // 2
    line = lax.broadcasted_iota(jnp.int32, (coarse_rows, columns), 0)
    for z in range(depth_half):
        for channel in range(channels):
            slot = (z * channels + channel) % result.shape[0]
            result[slot] = (
                totals[channel, 2 * z + 1] + totals[channel, 2 * z] + totals[channel, 2 * z + 2]
            )
            even = result[slot, pl.ds(0, coarse_rows, stride=2), :]
            odd = 0.5 * result[slot, pl.ds(1, coarse_rows, stride=2), :]
            across[slot, PAD : PAD + coarse_rows, :] = odd
            tail = jnp.where(line == coarse_rows - 1, odd, 0.0)
            value = even + odd + across[slot, PAD - 1 : PAD - 1 + coarse_rows, :] + tail
            at, side = (channel % half) * coarse_rows, channel // half * columns
            blocks[z, at : at + coarse_rows, side : side + columns] = value
        packed[z] = exact_dot(blocks[z], gather_pair)
    for j in range(shots):
        start = (shot_index ^ j) * share
        for k in range(half):
            for z in range(depth_half):
                at = (k * depth_half + z) * share
                chunks[j][at : at + share, :] = packed[z, pl.ds(k * coarse_rows + start, share), :]


def finish(*refs, steps):
    parts, out_ref = refs[:-1], refs[-1]
    channels, depth_len, share, columns = out_ref.shape
    total = parts[0][...]
    for part in parts[1:]:
        total = total + part[...]
    total = total / steps
    half = channels // 2
    for k in range(half):
        for z in range(depth_len):
            at = (k * depth_len + z) * share
            out_ref[k, z] = total[at : at + share, 0:columns]
            out_ref[k + half, z] = total[at : at + share, columns:]


def local_part(
    forward, adjoint_last, adjoint_late, residuals, source_cells, receiver_cells, assignment, model
):
    steps = forward.shape[0]
    shots_here, depth_len, rows, columns = adjoint_last.shape
    channels, coarse_len, share, coarse_columns = model.shape
    shots = lax.axis_size("shot")
    depth_count = lax.axis_size("depth")
    reach = (steps + 1) // 2
    assert shots_here == 1 and depth_count % 2 == 0 and shots & (shots - 1) == 0
    assert channels == 6 and 2 * coarse_columns == columns
    assert shots > 2 and steps % 2 == 0 and steps > 2 and depth_len > steps and coarse_len >= reach and share * shots * 2 == rows
    f32 = jnp.float32
    shape = lambda *dims: jax.ShapeDtypeStruct(dims, f32)
    local = lambda *dims: pltpu.VMEM(dims, f32)
    near = lambda array: pltpu.with_memory_space_constraint(array, pltpu.VMEM)
    far = lambda array: pltpu.with_memory_space_constraint(array, pltpu.HBM)
    first_pairs = [(i, i ^ 1) for i in range(depth_count)]
    second_pairs = [(i, (i + 1 if i % 2 else i - 1) % depth_count) for i in range(depth_count)]

    def moved(array, axis, pairs):
        return near(lax.ppermute(array, axis, pairs))

    half = channels // 2
    part = reach * half * share
    own_rows = coarse_len * half * share
    halo = 3 * steps + 1
    own, model_first, model_second, field_first, field_second = pl.pallas_call(
        functools.partial(pack, steps=steps, reach=reach),
        in_specs=[HBM] * 4,
        out_specs=[VMEM] * 5,
        out_shape=[local(own_rows, columns), local(part, columns), local(part, columns)]
        + [local(halo, rows, columns)] * 2,
        scratch_shapes=[
            local(*model.shape),
            pltpu.VMEM((steps, rows, columns), jnp.bfloat16),
            pltpu.SemaphoreType.DMA((6,)),
        ],
        name="pack",
        compiler_params=LIMIT,
    )(far(model), far(adjoint_last), far(adjoint_late), far(forward))
    model_second = moved(model_second, "depth", second_pairs)
    model_first = moved(model_first, "depth", first_pairs)
    field_second = moved(field_second, "depth", second_pairs)
    field_first = moved(field_first, "depth", first_pairs)
    height = depth_len + 2 * steps + 1
    added, keep, *loaded = pl.pallas_call(
        functools.partial(
            injection, steps=steps, depth_len=depth_len, rows=rows, depth_count=depth_count
        ),
        in_specs=[HBM] * 7,
        out_specs=[VMEM] * 5,
        out_shape=[
            local(steps, height - 2, rows, columns),
            local(depth_len + 1, rows, columns),
            local(1, depth_len, rows, columns),
            local(1, depth_len, rows, columns),
            pltpu.VMEM(forward.shape, forward.dtype),
        ],
        scratch_shapes=[
            pltpu.SMEM(assignment.shape, jnp.int32),
            pltpu.SMEM(source_cells.shape, jnp.int32),
            local(*residuals.shape),
            pltpu.VMEM((receiver_cells.shape[2],) + receiver_cells.shape[:2], jnp.int32),
            pltpu.SemaphoreType.DMA((7,)),
        ],
        name="injection",
        compiler_params=LIMIT,
    )(
        far(assignment),
        far(source_cells),
        far(residuals),
        far(receiver_cells.transpose(2, 0, 1)),
        far(adjoint_last),
        far(adjoint_late),
        far(forward),
    )
    joined_rows = own_rows + 2 * part
    joined = pl.pallas_call(
        functools.partial(join_model, layer=half * share, depth_count=depth_count),
        in_specs=[VMEM] * 3,
        out_specs=VMEM,
        out_shape=local(joined_rows, columns),
        name="join_model",
        compiler_params=LIMIT,
    )(near(own), model_first, model_second)
    swap = lambda array, j: moved(array, "shot", [(i, i ^ j) for i in range(shots)])
    gathered = [near(joined)] + [swap(joined, j) for j in range(1, shots)]
    padded = rows + 2 * PAD
    prepared = pl.pallas_call(
        functools.partial(prepare, steps=steps, depth_count=depth_count),
        in_specs=[VMEM] * 7,
        out_specs=[VMEM] * 5,
        out_shape=[
            local(height, padded, columns),
            local(channels, height - 2, rows, columns),
            local(height - 2, rows, columns),
            local(channels, depth_len + 1, rows, columns),
            local(steps, depth_len + 1, rows, columns),
        ],
        scratch_shapes=[
            local(height, padded, columns),
            local(height, rows, columns),
            local(height, rows, columns),
            local(height, rows, columns),
            local(height, rows, columns),
        ],
        name="prepare",
        compiler_params=LIMIT,
    )(
        *map(near, loaded),
        field_first,
        field_second,
        near(added),
        near(keep),
    )
    early = pl.pallas_call(
        refine_early,
        in_specs=[VMEM] * (shots - 2),
        out_specs=VMEM,
        out_shape=local(shots - 2, joined_rows, 2 * columns),
        name="refine_early",
        compiler_params=LIMIT,
    )(gathered[0], *gathered[3:])
    layers = coarse_len + 2 * reach
    chunk = local(half * coarse_len * share, columns)
    lines = [
        local(height, padded, columns),
        local(height, rows, columns),
        local(height, rows, columns),
        local(height, rows, columns),
    ]
    outs = pl.pallas_call(
        functools.partial(march, steps=steps, shots=shots, depth_count=depth_count, reach=reach),
        in_specs=[VMEM] * 9,
        out_specs=[VMEM] * (shots + 4),
        out_shape=[chunk] * shots
        + [
            local(height, padded, columns),
            local(height, padded, columns),
            local(layers, channels, rows, columns),
            local(layers - 1, channels, rows, columns),
        ],
        scratch_shapes=[
            local(coarse_len, half * rows // 2, 2 * columns),
            local(coarse_len, half * rows // 2, columns),
            local(layers, channels, rows // 2 + PAD, columns),
            *lines,
            local(channels, depth_len + 1, rows, columns),
            local(12, rows, columns),
        ],
        name="march",
        compiler_params=LIMIT,
    )(*map(near, prepared), near(added), near(early), *gathered[1:3])
    chunks, kept = outs[:shots], outs[shots:]
    final = pl.pallas_call(
        functools.partial(last_update, steps=steps, reach=reach),
        in_specs=[VMEM] * 5,
        out_specs=VMEM,
        out_shape=shape(1, depth_len, rows, columns),
        scratch_shapes=lines,
        name="last_update",
        compiler_params=LIMIT,
    )(*map(near, kept), near(added))
    parts = [near(chunks[0])] + [swap(chunks[j], j) for j in range(1, shots)]
    gradients = pl.pallas_call(
        functools.partial(finish, steps=steps),
        in_specs=[VMEM] * shots,
        out_specs=VMEM,
        out_shape=shape(*model.shape),
        name="finish",
        compiler_params=LIMIT,
    )(*parts)
    return final, gradients


def solution(mesh):
    placed = (
        P(None, ("grp", "shot"), "depth", None, None),
        P(("grp", "shot"), "depth", None, None),
        P(("grp", "shot"), "depth", None, None),
        P(("grp", "shot"), None, None),
        P("grp", None),
        P("grp", None, None),
        P("grp"),
        P(None, ("grp", "depth"), "shot", None),
    )
    return jax.shard_map(
        local_part,
        mesh=mesh,
        in_specs=placed,
        out_specs=(
            P(("grp", "shot"), "depth", None, None),
            P(None, ("grp", "depth"), "shot", None),
        ),
        check_vma=False,
    )
```

```python
import functools

import jax
import jax.numpy as jnp
from jax import lax
from jax.experimental import pallas as pl
from jax.experimental.pallas import tpu as pltpu
from jax.sharding import PartitionSpec as P

MUTE = 3
TIME_SQUARED = 0.2
PAD = 8
VMEM = pl.BlockSpec(memory_space=pltpu.VMEM)
SMEM = pl.BlockSpec(memory_space=pltpu.SMEM)
HBM = pl.BlockSpec(memory_space=pltpu.HBM)
LIMIT = pltpu.CompilerParams(vmem_limit_bytes=16 * 1024 * 1024)


def refine_matrix(coarse):
    row = lax.broadcasted_iota(jnp.int32, (coarse, 2 * coarse), 0)
    column = lax.broadcasted_iota(jnp.int32, (coarse, 2 * coarse), 1)
    here = column // 2
    after = jnp.minimum(here + 1, coarse - 1)
    odd = (column % 2) == 1
    at_here = jnp.where(row == here, 1.0, 0.0)
    at_after = jnp.where(row == after, 1.0, 0.0)
    return jnp.where(odd, 0.5 * (at_here + at_after), at_here).astype(jnp.float32)


def exact_dot(left, right):
    right = right.astype(jnp.bfloat16)
    parts = []
    for _ in range(3):
        parts.append(left.astype(jnp.bfloat16))
        left = left - parts[-1].astype(jnp.float32)
    product = functools.partial(jnp.dot, preferred_element_type=jnp.float32)
    if right.shape[0] == 128:
        stacked = jnp.concatenate([right, right], axis=0)
        return product(jnp.concatenate(parts[:2], axis=1), stacked) + product(parts[2], right)
    return product(parts[0], right) + product(parts[1], right) + product(parts[2], right)


def pair_matrix(coarse):
    refine = refine_matrix(coarse)
    none = jnp.zeros_like(refine)
    return jnp.concatenate(
        [jnp.concatenate([refine, none], axis=1), jnp.concatenate([none, refine], axis=1)], axis=0
    )


def refine_early(*refs):
    blocks, out_ref = refs[:-1], refs[-1]
    matrix = pair_matrix(blocks[0].shape[1] // 2)
    for j, block in enumerate(blocks):
        out_ref[j] = exact_dot(block[...], matrix)


def even_depth():
    return lax.axis_index("depth") % 2 == 0


def pack(
    model_ref,
    current_ref,
    previous_ref,
    forward_ref,
    own_ref,
    model_first,
    model_second,
    field_first,
    field_second,
    block,
    weights,
    sems,
    *,
    steps,
    reach,
):
    channels, coarse_len, share, coarse_columns = model_ref.shape
    half = channels // 2
    depth_len = current_ref.shape[1]
    up, down = steps + 1, steps
    part = reach * half * share
    total = coarse_len * half * share
    model_copy = pltpu.make_async_copy(model_ref, block, sems.at[5])
    model_copy.start()

    def fill(bottom, top, model_bottom, model_top):
        copies = [
            pltpu.make_async_copy(forward_ref.at[:, 0, depth_len - 1], weights, sems.at[0]),
            pltpu.make_async_copy(
                current_ref.at[0, depth_len - up : depth_len], bottom.at[0:up], sems.at[1]
            ),
            pltpu.make_async_copy(
                previous_ref.at[0, depth_len - up + 1 : depth_len],
                bottom.at[up : 2 * up - 1],
                sems.at[2],
            ),
            pltpu.make_async_copy(current_ref.at[0, 0:down], top.at[0:down], sems.at[3]),
            pltpu.make_async_copy(
                previous_ref.at[0, 0 : down - 1], top.at[down : 2 * down - 1], sems.at[4]
            ),
        ]
        for copy in copies:
            copy.start()
        model_copy.wait()
        for z in range(coarse_len):
            for k in range(half):
                at = (z * half + k) * share
                own_ref[at : at + share, 0:coarse_columns] = block[k, z]
                own_ref[at : at + share, coarse_columns:] = block[k + half, z]
        model_bottom[...] = own_ref[total - part : total, :]
        model_top[...] = own_ref[0:part, :]
        copies[0].wait()
        for i in range(steps):
            bottom[2 * up - 1 + i] = weights[i].astype(jnp.float32)
        for copy in copies[1:]:
            copy.wait()

    even = even_depth()

    @pl.when(even)
    def _():
        fill(field_first, field_second, model_first, model_second)

    @pl.when(jnp.logical_not(even))
    def _():
        fill(field_second, field_first, model_second, model_first)


def join_model(own_ref, first_ref, second_ref, out_ref, *, layer, depth_count):
    part = first_ref.shape[0]
    own = own_ref.shape[0]
    out_ref[part : part + own, :] = own_ref[...]
    even = even_depth()
    last = lax.axis_index("depth") == depth_count - 1

    @pl.when(even)
    def _():
        out_ref[0:part, :] = second_ref[...]
        out_ref[part + own : 2 * part + own, :] = first_ref[...]

    @pl.when(jnp.logical_not(even))
    def _():
        out_ref[0:part, :] = first_ref[...]
        out_ref[part + own : 2 * part + own, :] = second_ref[...]

    @pl.when(last)
    def _():
        out_ref[part + own : part + own + layer, :] = own_ref[own - layer : own, :]


def injection(
    assign_hbm,
    source_hbm,
    residual_hbm,
    receiver_hbm,
    current_ref,
    previous_ref,
    forward_ref,
    out_ref,
    keep_ref,
    current_out,
    previous_out,
    forward_out,
    assign_ref,
    source_ref,
    residual_ref,
    receiver_ref,
    sems,
    *,
    steps,
    depth_len,
    rows,
    depth_count,
):
    loads = [
        pltpu.make_async_copy(source, target, sems.at[n])
        for n, (source, target) in enumerate(
            [
                (assign_hbm, assign_ref),
                (source_hbm, source_ref),
                (receiver_hbm, receiver_ref),
                (residual_hbm, residual_ref),
                (current_ref, current_out),
                (previous_ref, previous_out),
                (forward_ref, forward_out),
            ]
        )
    ]
    for load in loads:
        load.start()
    for load in loads[:4]:
        load.wait()
    receivers = receiver_ref.shape[2]
    columns = out_ref.shape[3]
    count = out_ref.shape[1]
    geometry = assign_ref[lax.axis_index("shot")]
    first = lax.axis_index("depth") * depth_len - steps
    depth = receiver_ref[0, pl.ds(geometry, 1), :] - first
    flat = depth * rows + receiver_ref[1, pl.ds(geometry, 1), :]
    flat = jnp.where((depth >= 0) & (depth < count), flat, -1)
    cells = lax.broadcasted_iota(jnp.int32, (count * rows, receivers), 0)
    one_hot = jnp.where(cells == flat, 1.0, 0.0).astype(jnp.bfloat16)
    lanes = lax.broadcasted_iota(jnp.int32, (columns, receivers), 0)
    here = lanes == receiver_ref[2, pl.ds(geometry, 1), :]
    for i in range(steps):
        left = residual_ref[0, i : i + 1, :]
        total = None
        for _ in range(3):
            rounded = left.astype(jnp.bfloat16).astype(jnp.float32)
            left = left - rounded
            values = jnp.where(here, rounded, 0.0).astype(jnp.bfloat16)
            product = lax.dot_general(
                one_hot, values, (((1,), (1,)), ((), ())), preferred_element_type=jnp.float32
            )
            total = product if total is None else total + product
        out_ref[i] = total.reshape(count, rows, columns)

    depth_index = lax.axis_index("depth")
    row = lax.broadcasted_iota(jnp.int32, (rows, columns), 0)
    lane = lax.broadcasted_iota(jnp.int32, (rows, columns), 1)
    near = (jnp.abs(row - source_ref[geometry, 1]) <= MUTE) & (
        jnp.abs(lane - source_ref[geometry, 2]) <= MUTE
    )
    away = jnp.where(near, 0.0, 1.0)
    for e in range(depth_len + 1):
        close = jnp.abs(depth_index * depth_len + e - 1 - source_ref[geometry, 0]) <= MUTE
        if e == 0:
            scale = jnp.where(depth_index == 0, 0.0, 0.5)
        elif e == depth_len:
            scale = jnp.where(depth_index == depth_count - 1, 1.0, 0.5)
        else:
            scale = 1.0 if e % 2 else 0.5
        keep_ref[e] = jnp.where(close, away, 1.0) * scale
    for load in loads[4:]:
        load.wait()


def slopes_at(field, lines, e, rows):
    across, bend, slant, bow = lines
    inner = slice(PAD, PAD + rows)
    before = slice(PAD - 1, PAD - 1 + rows)
    after = slice(PAD + 1, PAD + 1 + rows)
    twice = 2.0 * field[e, inner, :]
    slopes = [
        field[e + 1, inner, :] - twice + field[e - 1, inner, :],
        bow[e],
        bend[e],
        slant[e + 1] - slant[e - 1],
        across[e + 1, inner, :] - across[e - 1, inner, :],
        across[e, after, :] - across[e, before, :],
    ]
    return twice, slopes


def differences(field, lines, lowest, highest, rows):
    across, bend, slant, bow = lines
    columns = field.shape[2]
    inner = slice(PAD, PAD + rows)
    lane = lax.broadcasted_iota(jnp.int32, (rows, columns), 1)
    for e in range(lowest, highest + 1):
        value = field[e, inner, :]
        twice = 2.0 * value
        right = jnp.where(lane == columns - 1, 0.0, pltpu.roll(value, columns - 1, 1))
        left = jnp.where(lane == 0, 0.0, pltpu.roll(value, 1, 1))
        across[e, inner, :] = right - left
        bend[e] = right + left - twice
        before = field[e, PAD - 1 : PAD - 1 + rows, :]
        after = field[e, PAD + 1 : PAD + 1 + rows, :]
        slant[e] = after - before
        if lowest < e < highest:
            bow[e] = after + before - twice


def clear_rim(field, rows):
    height, _, columns = field.shape
    rim = jnp.zeros((height, PAD, columns), jnp.float32)
    field[:, 0:PAD, :] = rim
    field[:, PAD + rows : 2 * PAD + rows, :] = rim


def prepare(
    current_ref,
    previous_ref,
    forward_ref,
    first_ref,
    second_ref,
    added_ref,
    keep_ref,
    field,
    start_slopes,
    start_base,
    start_totals,
    weights,
    across,
    bend,
    slant,
    bow,
    older,
    *,
    steps,
    depth_count,
):
    depth_len, rows, _ = current_ref.shape[1:]
    up, down = steps + 1, steps
    height = up + depth_len + down
    depth_index = lax.axis_index("depth")
    is_even = depth_index % 2 == 0
    inner = slice(PAD, PAD + rows)
    clear_rim(field, rows)
    clear_rim(across, rows)
    field[up : up + depth_len, inner, :] = current_ref[0]
    older[up : up + depth_len] = previous_ref[0]
    for i in range(steps):
        weights[i, 1 : depth_len + 1] = (
            forward_ref[i, 0].astype(jnp.float32) * keep_ref[1 : depth_len + 1]
        )

    def from_above(ref):
        field[0:up, inner, :] = ref[0:up]
        older[1:up] = ref[up : 2 * up - 1]
        for i in range(steps):
            weights[i, 0] = ref[2 * up - 1 + i] * keep_ref[0]

    def from_below(ref):
        field[up + depth_len : height, inner, :] = ref[0:down]
        older[up + depth_len : height - 1] = ref[down : 2 * down - 1]

    @pl.when(is_even)
    def _():
        from_above(second_ref)
        from_below(first_ref)

    @pl.when(jnp.logical_not(is_even))
    def _():
        from_above(first_ref)
        from_below(second_ref)

    @pl.when(depth_index == 0)
    def _():
        field[0:up, inner, :] = jnp.zeros((up,) + current_ref.shape[2:], jnp.float32)
        older[0:up] = jnp.zeros((up,) + current_ref.shape[2:], jnp.float32)

    @pl.when(depth_index == depth_count - 1)
    def _():
        field[up + depth_len : height, inner, :] = jnp.zeros(
            (down,) + current_ref.shape[2:], jnp.float32
        )
        older[up + depth_len : height] = jnp.zeros((down,) + current_ref.shape[2:], jnp.float32)

    lines = (across, bend, slant, bow)
    differences(field, lines, 0, height - 1, rows)
    for e in range(1, height - 1):
        twice, slopes = slopes_at(field, lines, e, rows)
        for k, slope in enumerate(slopes):
            start_slopes[k, e - 1] = slope
            if up - 1 <= e < up + depth_len:
                start_totals[k, e - up + 1] = weights[0, e - up + 1] * slope
        start_base[e - 1] = twice - older[e] + added_ref[0, e - 1]


def change_at(even_rows, odd_rows, slopes, z):
    table = even_rows if z % 2 == 0 else odd_rows
    change = table[z // 2, 0] * slopes[0]
    for k in range(1, len(slopes)):
        change = change + table[z // 2, k] * slopes[k]
    return change


def last_update(*refs, steps, reach):
    now, old, even_rows, odd_rows, added_ref, final_ref, *lines = refs
    depth_len, rows, _ = final_ref.shape[1:]
    up = steps + 1
    clear_rim(lines[0], rows)
    differences(now, lines, up - 1, up + depth_len, rows)
    for e in range(up, up + depth_len):
        twice, slopes = slopes_at(now, lines, e, rows)
        base = twice - old[e, PAD : PAD + rows, :] + added_ref[steps - 1, e - 1]
        final_ref[0, e - up] = base + change_at(even_rows, odd_rows, slopes, e - up + 2 * reach)


def march(
    field,
    start_slopes,
    start_base,
    start_totals,
    weights,
    added_ref,
    *refs,
    steps,
    shots,
    depth_count,
    reach,
):
    early_ref, *refs = refs
    late, refs = refs[:2], refs[2:]
    chunks = refs[:shots]
    ones, twos, even_rows, odd_rows, blocks, packed, coarse, *lines, totals, result = refs[
        shots:
    ]
    across = lines[0]
    rows, columns = start_base.shape[1:]
    channels, depth_len = start_slopes.shape[0], weights.shape[1] - 1
    up, down = steps + 1, steps
    height = up + depth_len + down
    depth_index = lax.axis_index("depth")
    shot_index = lax.axis_index("shot")
    is_top = depth_index == 0
    is_last = depth_index == depth_count - 1
    coarse_rows = rows // 2
    share = coarse_rows // shots
    layers = depth_len // 2 + 2 * reach
    inner = slice(PAD, PAD + rows)
    for scratch in (ones, twos, across):
        clear_rim(scratch, rows)

    half = channels // 2
    refine = refine_matrix(columns // 2)
    matrix = pair_matrix(columns // 2)
    for j in range(shots):
        wide = exact_dot(late[j - 1][...], matrix) if j in (1, 2) else early_ref[max(j - 2, 0)]
        start = (shot_index ^ j) * share
        for z in range(layers):
            for k in range(half):
                at = (z * half + k) * share
                for side in range(2):
                    coarse[z, k + side * half, pl.ds(start, share), :] = wide[
                        at : at + share, side * columns : (side + 1) * columns
                    ]
    for z in range(layers):
        for k in range(channels):
            coarse[z, k, coarse_rows : coarse_rows + 1, :] = coarse[
                z, k, coarse_rows - 1 : coarse_rows, :
            ]
            scale = TIME_SQUARED if k < 3 else 0.25 * TIME_SQUARED
            here = coarse[z, k, 0:coarse_rows, :]
            after = coarse[z, k, 1 : coarse_rows + 1, :]
            even_rows[z, k, pl.ds(0, coarse_rows, stride=2), :] = here * scale
            even_rows[z, k, pl.ds(1, coarse_rows, stride=2), :] = (here + after) * (0.5 * scale)
    for z in range(layers - 1):
        for k in range(channels):
            odd_rows[z, k] = (even_rows[z, k] + even_rows[z + 1, k]) * 0.5

    for i in range(steps):
        now = field if i == 0 else (ones if i % 2 else twos)
        old = field if i == 1 else (twos if i % 2 else ones)
        new = twos if i % 2 else ones
        last = i == steps - 1
        if i > 0:
            differences(now, lines, i, height - 1 - i, rows)
        for e in range(i + 1, height - 1 - i):
            counted = up - 1 <= e < up + depth_len and i > 0
            if last and not counted:
                continue
            if i == 0:
                slopes = [start_slopes[k, e - 1] for k in range(channels)]
                base = start_base[e - 1]
            else:
                twice, slopes = slopes_at(now, lines, e, rows)
            if counted:
                weight = weights[i, e - up + 1]
                for k in range(channels):
                    so_far = start_totals if i == 1 else totals
                    totals[k, e - up + 1] = so_far[k, e - up + 1] + weight * slopes[k]
            if not last:
                if i > 0:
                    base = twice - old[e, inner, :] + added_ref[i, e - 1]
                updated = base + change_at(even_rows, odd_rows, slopes, e - up + 2 * reach)
                if e < up:
                    updated = jnp.where(is_top, 0.0, updated)
                if e >= up + depth_len:
                    updated = jnp.where(is_last, 0.0, updated)
                new[e, inner, :] = updated

    gather = refine.T
    none = jnp.zeros_like(gather)
    gather_pair = jnp.concatenate(
        [
            jnp.concatenate([gather, none], axis=1),
            jnp.concatenate([none, 0.25 * gather], axis=1),
        ],
        axis=0,
    )
    depth_half = depth_len // 2
    line = lax.broadcasted_iota(jnp.int32, (coarse_rows, columns), 0)
    for z in range(depth_half):
        for channel in range(channels):
            slot = (z * channels + channel) % result.shape[0]
            result[slot] = (
                totals[channel, 2 * z + 1] + totals[channel, 2 * z] + totals[channel, 2 * z + 2]
            )
            even = result[slot, pl.ds(0, coarse_rows, stride=2), :]
            odd = 0.5 * result[slot, pl.ds(1, coarse_rows, stride=2), :]
            across[slot, PAD : PAD + coarse_rows, :] = odd
            tail = jnp.where(line == coarse_rows - 1, odd, 0.0)
            value = even + odd + across[slot, PAD - 1 : PAD - 1 + coarse_rows, :] + tail
            at, side = (channel % half) * coarse_rows, channel // half * columns
            blocks[z, at : at + coarse_rows, side : side + columns] = value
        packed[z] = exact_dot(blocks[z], gather_pair)
    for j in range(shots):
        start = (shot_index ^ j) * share
        for k in range(half):
            for z in range(depth_half):
                at = (k * depth_half + z) * share
                chunks[j][at : at + share, :] = packed[z, pl.ds(k * coarse_rows + start, share), :]


def finish(*refs, steps):
    parts, out_ref = refs[:-1], refs[-1]
    channels, depth_len, share, columns = out_ref.shape
    total = parts[0][...]
    for part in parts[1:]:
        total = total + part[...]
    total = total / steps
    half = channels // 2
    for k in range(half):
        for z in range(depth_len):
            at = (k * depth_len + z) * share
            out_ref[k, z] = total[at : at + share, 0:columns]
            out_ref[k + half, z] = total[at : at + share, columns:]


def local_part(
    forward, adjoint_last, adjoint_late, residuals, source_cells, receiver_cells, assignment, model
):
    steps = forward.shape[0]
    shots_here, depth_len, rows, columns = adjoint_last.shape
    channels, coarse_len, share, coarse_columns = model.shape
    shots = lax.axis_size("shot")
    depth_count = lax.axis_size("depth")
    reach = (steps + 1) // 2
    assert shots_here == 1 and depth_count % 2 == 0 and shots & (shots - 1) == 0
    assert channels == 6 and 2 * coarse_columns == columns
    assert shots > 2 and steps % 2 == 0 and steps > 2 and depth_len > steps and coarse_len >= reach and share * shots * 2 == rows
    f32 = jnp.float32
    shape = lambda *dims: jax.ShapeDtypeStruct(dims, f32)
    local = lambda *dims: pltpu.VMEM(dims, f32)
    near = lambda array: pltpu.with_memory_space_constraint(array, pltpu.VMEM)
    far = lambda array: pltpu.with_memory_space_constraint(array, pltpu.HBM)
    first_pairs = [(i, i ^ 1) for i in range(depth_count)]
    second_pairs = [(i, (i + 1 if i % 2 else i - 1) % depth_count) for i in range(depth_count)]

    def moved(array, axis, pairs):
        return near(lax.ppermute(array, axis, pairs))

    half = channels // 2
    part = reach * half * share
    own_rows = coarse_len * half * share
    halo = 3 * steps + 1
    own, model_first, model_second, field_first, field_second = pl.pallas_call(
        functools.partial(pack, steps=steps, reach=reach),
        in_specs=[HBM] * 4,
        out_specs=[VMEM] * 5,
        out_shape=[local(own_rows, columns), local(part, columns), local(part, columns)]
        + [local(halo, rows, columns)] * 2,
        scratch_shapes=[
            local(*model.shape),
            pltpu.VMEM((steps, rows, columns), jnp.bfloat16),
            pltpu.SemaphoreType.DMA((6,)),
        ],
        name="pack",
        compiler_params=LIMIT,
    )(far(model), far(adjoint_last), far(adjoint_late), far(forward))
    model_second = moved(model_second, "depth", second_pairs)
    model_first = moved(model_first, "depth", first_pairs)
    field_second = moved(field_second, "depth", second_pairs)
    field_first = moved(field_first, "depth", first_pairs)
    height = depth_len + 2 * steps + 1
    added, keep, *loaded = pl.pallas_call(
        functools.partial(
            injection, steps=steps, depth_len=depth_len, rows=rows, depth_count=depth_count
        ),
        in_specs=[HBM] * 7,
        out_specs=[VMEM] * 5,
        out_shape=[
            local(steps, height - 2, rows, columns),
            local(depth_len + 1, rows, columns),
            local(1, depth_len, rows, columns),
            local(1, depth_len, rows, columns),
            pltpu.VMEM(forward.shape, forward.dtype),
        ],
        scratch_shapes=[
            pltpu.SMEM(assignment.shape, jnp.int32),
            pltpu.SMEM(source_cells.shape, jnp.int32),
            local(*residuals.shape),
            pltpu.VMEM((receiver_cells.shape[2],) + receiver_cells.shape[:2], jnp.int32),
            pltpu.SemaphoreType.DMA((7,)),
        ],
        name="injection",
        compiler_params=LIMIT,
    )(
        far(assignment),
        far(source_cells),
        far(residuals),
        far(receiver_cells.transpose(2, 0, 1)),
        far(adjoint_last),
        far(adjoint_late),
        far(forward),
    )
    joined_rows = own_rows + 2 * part
    joined = pl.pallas_call(
        functools.partial(join_model, layer=half * share, depth_count=depth_count),
        in_specs=[VMEM] * 3,
        out_specs=VMEM,
        out_shape=local(joined_rows, columns),
        name="join_model",
        compiler_params=LIMIT,
    )(near(own), model_first, model_second)
    swap = lambda array, j: moved(array, "shot", [(i, i ^ j) for i in range(shots)])
    gathered = [near(joined)] + [swap(joined, j) for j in range(1, shots)]
    padded = rows + 2 * PAD
    prepared = pl.pallas_call(
        functools.partial(prepare, steps=steps, depth_count=depth_count),
        in_specs=[VMEM] * 7,
        out_specs=[VMEM] * 5,
        out_shape=[
            local(height, padded, columns),
            local(channels, height - 2, rows, columns),
            local(height - 2, rows, columns),
            local(channels, depth_len + 1, rows, columns),
            local(steps, depth_len + 1, rows, columns),
        ],
        scratch_shapes=[
            local(height, padded, columns),
            local(height, rows, columns),
            local(height, rows, columns),
            local(height, rows, columns),
            local(height, rows, columns),
        ],
        name="prepare",
        compiler_params=LIMIT,
    )(
        *map(near, loaded),
        field_first,
        field_second,
        near(added),
        near(keep),
    )
    early = pl.pallas_call(
        refine_early,
        in_specs=[VMEM] * (shots - 2),
        out_specs=VMEM,
        out_shape=local(shots - 2, joined_rows, 2 * columns),
        name="refine_early",
        compiler_params=LIMIT,
    )(gathered[0], *gathered[3:])
    layers = coarse_len + 2 * reach
    chunk = local(half * coarse_len * share, columns)
    lines = [
        local(height, padded, columns),
        local(height, rows, columns),
        local(height, rows, columns),
        local(height, rows, columns),
    ]
    outs = pl.pallas_call(
        functools.partial(march, steps=steps, shots=shots, depth_count=depth_count, reach=reach),
        in_specs=[VMEM] * 9,
        out_specs=[VMEM] * (shots + 4),
        out_shape=[chunk] * shots
        + [
            local(height, padded, columns),
            local(height, padded, columns),
            local(layers, channels, rows, columns),
            local(layers - 1, channels, rows, columns),
        ],
        scratch_shapes=[
            local(coarse_len, half * rows // 2, 2 * columns),
            local(coarse_len, half * rows // 2, columns),
            local(layers, channels, rows // 2 + PAD, columns),
            *lines,
            local(channels, depth_len + 1, rows, columns),
            local(12, rows, columns),
        ],
        name="march",
        compiler_params=LIMIT,
    )(*map(near, prepared), near(added), near(early), *gathered[1:3])
    chunks, kept = outs[:shots], outs[shots:]
    final = pl.pallas_call(
        functools.partial(last_update, steps=steps, reach=reach),
        in_specs=[VMEM] * 5,
        out_specs=VMEM,
        out_shape=shape(1, depth_len, rows, columns),
        scratch_shapes=lines,
        name="last_update",
        compiler_params=LIMIT,
    )(*map(near, kept), near(added))
    parts = [near(chunks[0])] + [swap(chunks[j], j) for j in range(1, shots)]
    gradients = pl.pallas_call(
        functools.partial(finish, steps=steps),
        in_specs=[VMEM] * shots,
        out_specs=VMEM,
        out_shape=shape(*model.shape),
        name="finish",
        compiler_params=LIMIT,
    )(*parts)
    return final, gradients


def solution(mesh):
    placed = (
        P(None, ("grp", "shot"), "depth", None, None),
        P(("grp", "shot"), "depth", None, None),
        P(("grp", "shot"), "depth", None, None),
        P(("grp", "shot"), None, None),
        P("grp", None),
        P("grp", None, None),
        P("grp"),
        P(None, ("grp", "depth"), "shot", None),
    )
    return jax.shard_map(
        local_part,
        mesh=mesh,
        in_specs=placed,
        out_specs=(
            P(("grp", "shot"), "depth", None, None),
            P(None, ("grp", "depth"), "shot", None),
        ),
        check_vma=False,
    )
```
